256 devices in a mesh: dp: 8 (over z_hi, core), row: 8 (over y, z_lo), col: 4 (over x).
Axes of the slice: x: 4, y: 4, z: 8 (z_hi: 4, z_lo: 2; z = z_hi * 2 + z_lo), core: 2. Of those that a mesh axis runs over, the one named last changes fastest.
Arguments:
- activations: bfloat16 [8192, 4096], P('dp', 'col'), may hold values from -6 to 6
- out_grad: bfloat16 [8192, 14336], P('dp', 'row'), may hold values from -6 to 6
- weight: float32 [8, 1792, 4096], P('row', 'dp', 'col'), as said below
- step_size: float32 [8, 1792], P('row'), may hold values from 0.001 to 0.016
Outputs:
- input_grad: bfloat16 [8192, 4096], P(('dp', 'row'), 'col')
- weight_grad: float32 [8, 1792, 4096], P('row', 'dp', 'col')
- step_grad: float32 [8, 1792], P('row', 'dp')
The draws below stay inside these ranges and needn't reach their ends.
Inputs may be any that keep to these rules, and one draw needn't show every extreme that they name: Each latent weight divided by its row's step lies at least 0.1 away from every multiple of one half.
All inputs are finite; a program needn't handle non-finite values.
Results may differ from the reference program's by a relative error of at most 0.0096.
Values may be sent and summed in bfloat16 or wider, within the bound.
A program may use at most 128 MiB of HBM per device.

```python
import jax
import jax.numpy as jnp
from jax import lax

D = 4096
FF = 14336
TOKENS = 8192
N_ROW = 8


def joint_draw(key):
    base = jax.random.fold_in(key, 7)
    first, second, third, fourth = jax.random.split(base, 4)
    logs = jax.random.uniform(first, (N_ROW, FF // N_ROW), jnp.float32, jnp.log(0.002), jnp.log(0.008))
    scales = jnp.exp(logs)
    codes = jax.random.randint(second, (N_ROW, FF // N_ROW, D), -10, 10).astype(jnp.float32)
    magnitudes = jax.random.uniform(third, (N_ROW, FF // N_ROW, D), jnp.float32, 0.1, 0.4)
    signs = jnp.where(jax.random.bernoulli(fourth, 0.5, (N_ROW, FF // N_ROW, D)), 1.0, -1.0)
    latent = scales[:, :, None] * (codes + signs * magnitudes)
    return (scales, latent)


def draw_weight(key, part):
    scales, latent = joint_draw(key)
    return latent.astype(jnp.float32)


def draw_step_size(key, part):
    scales, latent = joint_draw(key)
    return scales.astype(jnp.float32)


def with_spikes(values, own_key, source, target, blocks, factor):
    owner, partner = [(jnp.arange(values.shape[position]) // (values.shape[position] // blocks)).reshape([-1 if axis == position else 1 for axis in range(values.ndim)]) for position in (source, target)]
    chosen = jax.random.permutation(own_key, blocks)[partner]
    strong = (owner == chosen) | (owner == (partner + blocks // 2) % blocks)
    return jnp.where(strong, factor * values, values)


def level_of(stream_key, shape, shards, smallest, top_value):
    def one(axis_at, shards_of):
        heights = jax.random.uniform(jax.random.fold_in(jax.random.fold_in(stream_key, 6), axis_at), (shards_of,), jnp.float32, smallest / len(shards), top_value / len(shards))
        return jnp.repeat(jnp.exp(heights), shape[axis_at] // shards_of).reshape((-1,) + (1,) * (len(shape) - axis_at - 1))

    level = one(*shards[0])
    for cut in shards[1:]:
        level = level * one(*cut)
    return level


def noise(key, dims, spread, bound, cuts=(), held_as=jnp.bfloat16):
    entries = jax.random.normal(key, dims, jnp.float32) * spread
    if len(cuts) > 0:
        entries = level_of(key, dims, cuts, -0.22, 0.18) * entries
    return jnp.clip(entries, min=-bound, max=bound).astype(held_as)


def heavy_noise(key, dims, spread, limit, shards, heavy, held_as=jnp.bfloat16):
    drawn = spread * jax.random.normal(key, dims, jnp.float32)
    if shards:
        drawn = drawn * level_of(key, dims, shards, -0.22, 0.18)
    return jnp.clip(with_spikes(drawn, jax.random.fold_in(key, 3), *heavy), -limit, limit).astype(held_as)


def setup_inputs(seed: int = 0) -> dict:
    arg_keys = jax.random.split(jax.random.key(seed), 5)
    activations = noise(arg_keys[0], (TOKENS, D), 1.0, 6.0, ((0, 8), (1, 4)))
    out_grad = heavy_noise(arg_keys[1], (TOKENS, FF), ((D / FF) ** 0.5), 6.0, ((0, 8), (1, 8)), (0, 1, 8, 2.0))
    weight = draw_weight(jax.random.fold_in(arg_keys[4], 71), 0)
    step_size = draw_step_size(jax.random.fold_in(arg_keys[4], 71), 0)
    return dict(activations=activations, out_grad=out_grad, weight=weight, step_size=step_size)


def reference(activations, out_grad, weight, step_size):
    scales = step_size.reshape(FF)
    latent = weight.reshape(FF, D)
    ratio = latent / scales[:, None]
    clipped = jnp.clip(ratio, -8.0, 7.0)
    levels = jnp.floor(clipped + 0.5)
    quantized = (levels * scales[:, None]).astype(jnp.bfloat16)
    inside = jnp.where((ratio >= -8.0) & (ratio <= 7.0), 1.0, 0.0).astype(jnp.float32)
    factor = jnp.where(inside > 0.5, levels - ratio, clipped)
    input_grad = jnp.dot(out_grad, quantized, preferred_element_type=jnp.float32).astype(jnp.bfloat16)
    products = lax.dot_general(out_grad, activations, (((0,), (0,)), ((), ())), preferred_element_type=jnp.float32)
    weight_grad = (products * inside).reshape(N_ROW, FF // N_ROW, D)
    grad_factor = 1.0 / (7.0 * D) ** 0.5
    step_grad = (jnp.sum(products * factor, axis=1) * grad_factor).reshape(N_ROW, FF // N_ROW)
    return input_grad, weight_grad, step_grad
```

```python
import functools

import jax
import jax.numpy as jnp
from jax import lax
from jax.experimental import pallas as pl
from jax.experimental.pallas import tpu as pltpu
from jax.sharding import Mesh
from jax.sharding import PartitionSpec as P

MESH = pl.DeviceIdType.MESH
D = 4096
DP = ("zh", "core")
ROW = ("y", "zl")
OWN = 224
HALF = 112
COLS = 1024
ROWS = 1792
TOKENS = 1024
SUB = 128
GRAD_FACTOR = 1.0 / (7.0 * D) ** 0.5

AG_RA, AG_RB, AG_LB, AG_LA, AG_FR, AG_FL = range(6)
D_OWN, D_LEFT, D_RIGHT, D_FAR = range(6, 10)
D_P = 10
RS_FR, RS_FL, RS_OR, RS_OL, RS_SR, RS_SL = range(14, 20)
Y_FU, Y_FD, Y_OU, Y_OD, Y_SU, Y_SD = range(20, 26)
Z_PAIR = 26
X_SUM = 27
N_COPIES = 30


def rows_of(index, size):
    return pl.ds(pl.multiple_of(index * size, size), size)


def kernel(
    act_hbm, og_hbm, w_hbm, s_hbm,
    ig_out, wg_out, sg_out,
    act, og, w, s, scol, ogt, q, fac, ins,
    p_own, p_snd, p_rcv, c_buf,
    rs_far, rs_own, rs_sum, rs_snd,
    g, gown, y_far, y_own, y_sum, y_snd, tot, z_snd, z_rcv,
    x_snd, x_rcv,
    ss, rs, ls,
):
    zh = lax.axis_index("zh")
    core = lax.axis_index("core")
    y = lax.axis_index("y")
    zl = lax.axis_index("zl")
    x = lax.axis_index("x")
    zr, zlft, zf = (zh + 1) % 4, (zh + 3) % 4, (zh + 2) % 4
    right, left = {"zh": zr}, {"zh": zlft}
    other = 1 - core
    peer = {"core": other}
    yu, yd, yf = (y + 1) % 4, (y + 3) % 4, (y + 2) % 4
    up, down = {"y": yu}, {"y": yd}
    pair = {"zl": 1 - zl}
    crosses = [{"x": (x + k) % 4} for k in (1, 2, 3)]

    loads = [
        pltpu.make_async_copy(w_hbm, w, ls.at[0]),
        pltpu.make_async_copy(s_hbm, s, ls.at[1]),
        pltpu.make_async_copy(og_hbm, og, ls.at[2]),
        pltpu.make_async_copy(act_hbm, act, ls.at[3]),
    ]
    for load in loads:
        load.start()

    barrier = pltpu.get_barrier_semaphore()
    partners = [right, left, peer, up, down, pair] + crosses
    for partner in partners:
        pl.semaphore_signal(barrier, inc=1, device_id=partner, device_id_type=MESH)

    def copy(src, dst, number, device):
        return pltpu.make_async_remote_copy(
            src_ref=src, dst_ref=dst, send_sem=ss.at[number], recv_sem=rs.at[number],
            device_id=device, device_id_type=MESH,
        )

    def shard(j, c):
        return q.at[rows_of(j * 2 + c, OWN)]

    def half(j, c, h):
        return q.at[rows_of((j * 2 + c) * 2 + h, HALF)]

    loads[1].wait()
    scol[...] = jnp.transpose(jnp.broadcast_to(s[...], (128, ROWS)))
    loads[0].wait()
    own_row = (zh * 2 + core) * OWN
    own_at = pl.ds(pl.multiple_of(own_row, OWN), OWN)
    scale = scol[own_at, :]
    for k in range(COLS // 128):
        at = slice(k * 128, (k + 1) * 128)
        ratio = w[:, at] / scale
        levels = jnp.floor(jnp.clip(ratio, -8.0, 7.0) + 0.5)
        q[own_at, at] = (levels * scale).astype(jnp.bfloat16)

    pl.semaphore_wait(barrier, len(partners))

    ag = {
        AG_RA: copy(half(zh, core, 0), half(zh, core, 0), AG_RA, right),
        AG_RB: copy(half(zh, core, 1), half(zh, core, 1), AG_RB, right),
        AG_LB: copy(half(zh, core, 1), half(zh, core, 1), AG_LB, left),
        AG_LA: copy(half(zh, core, 0), half(zh, core, 0), AG_LA, left),
        AG_FR: copy(half(zlft, core, 0), half(zlft, core, 0), AG_FR, right),
        AG_FL: copy(half(zr, core, 1), half(zr, core, 1), AG_FL, left),
        D_OWN: copy(shard(zh, core), shard(zh, core), D_OWN, peer),
        D_LEFT: copy(shard(zlft, core), shard(zlft, core), D_LEFT, peer),
        D_RIGHT: copy(shard(zr, core), shard(zr, core), D_RIGHT, peer),
        D_FAR: copy(shard(zf, core), shard(zf, core), D_FAR, peer),
    }
    for number in (AG_RA, AG_LB, AG_RB, AG_LA, D_OWN):
        ag[number].start()

    for k in range(COLS // 128):
        at = slice(k * 128, (k + 1) * 128)
        ratio = w[:, at] / scale
        clipped = jnp.clip(ratio, -8.0, 7.0)
        levels = jnp.floor(clipped + 0.5)
        inside = (ratio >= -8.0) & (ratio <= 7.0)
        ins[:, at] = jnp.where(inside, 1.0, 0.0)
        fac[:, at] = jnp.where(inside, levels - ratio, clipped)

    loads[2].wait()
    for k in range(ROWS // 128):
        at = slice(k * 128, (k + 1) * 128)
        ogt[at, :] = jnp.transpose(og[:, at])
    loads[3].wait()

    def product(j, c, n):
        return jnp.dot(
            ogt[rows_of(j * 2 + c, OWN), :], act[:, n * 256:(n + 1) * 256],
            preferred_element_type=jnp.float32,
        )

    def to_peer(j):
        return copy(
            p_snd.at[rows_of(j, OWN)], p_rcv.at[rows_of(j, OWN)], D_P + j, peer
        )

    @pl.loop(0, 4)
    def _(j):
        for n in range(4):
            p_snd[rows_of(j, OWN), n * 256:(n + 1) * 256] = product(j, other, n).astype(jnp.bfloat16)

        @pl.when(j >= 1)
        def _():
            to_peer(j - 1).start()

    @pl.loop(0, 4)
    def _(j):
        for n in range(4):
            p_own[rows_of(j, OWN), n * 256:(n + 1) * 256] = product(j, core, n)

        @pl.when(j == 0)
        def _():
            to_peer(3).start()

    ag[AG_RA].wait_recv()
    ag[AG_LB].wait_recv()
    ag[AG_FR].start()
    ag[AG_FL].start()

    @pl.loop(0, 4)
    def _(j):
        to_peer(j).wait_recv()
        at = rows_of(j, OWN)
        total = p_own[at, :] + p_rcv[at, :].astype(jnp.float32)
        p_own[at, :] = total
        c_buf[at, :] = total.astype(jnp.bfloat16)

    def c_half(j, h):
        return c_buf.at[rows_of(j * 2 + h, HALF)]

    red = {
        RS_FR: copy(c_half(zf, 0), rs_far.at[0], RS_FR, right),
        RS_FL: copy(c_half(zf, 1), rs_far.at[1], RS_FL, left),
        RS_OR: copy(c_half(zr, 1), rs_own.at[1], RS_OR, right),
        RS_OL: copy(c_half(zlft, 0), rs_own.at[0], RS_OL, left),
        RS_SR: copy(rs_snd.at[0], rs_sum.at[0], RS_SR, right),
        RS_SL: copy(rs_snd.at[1], rs_sum.at[1], RS_SL, left),
    }
    for number in (RS_FR, RS_FL, RS_OR, RS_OL):
        red[number].start()

    ag[AG_RB].wait_recv()
    ag[D_LEFT].start()
    ag[AG_LA].wait_recv()
    ag[D_RIGHT].start()
    ag[AG_FR].wait_recv()
    ag[AG_FL].wait_recv()
    ag[D_FAR].start()
    for number in (D_OWN, D_LEFT, D_RIGHT, D_FAR):
        ag[number].wait_recv()

    def g_half(j, h):
        return g.at[rows_of(j * 2 + h, SUB)]

    ig = {
        Y_FU: copy(g_half(yf, 0), y_far.at[0], Y_FU, up),
        Y_FD: copy(g_half(yf, 1), y_far.at[1], Y_FD, down),
        Y_OU: copy(g_half(yu, 1), y_own.at[1], Y_OU, up),
        Y_OD: copy(g_half(yd, 0), y_own.at[0], Y_OD, down),
        Y_SU: copy(y_snd.at[0], y_sum.at[0], Y_SU, up),
        Y_SD: copy(y_snd.at[1], y_sum.at[1], Y_SD, down),
    }

    def block(t, n):
        return jnp.dot(
            og[rows_of(t, 2 * SUB), :], q[:, n * 256:(n + 1) * 256],
            preferred_element_type=jnp.float32,
        )

    @pl.loop(0, 3)
    def _(k):
        t = jnp.where(k == 0, yf, jnp.where(k == 1, yu, yd))
        for n in range(4):
            g[rows_of(t, 2 * SUB), n * 256:(n + 1) * 256] = block(t, n).astype(jnp.bfloat16)

        @pl.when(k == 0)
        def _():
            ig[Y_FU].start()
            ig[Y_FD].start()

    ig[Y_OU].start()
    ig[Y_OD].start()
    for n in range(4):
        gown[:, n * 256:(n + 1) * 256] = block(y, n)

    red[RS_FR].wait_recv()
    rs_snd[0] = (
        p_own[rows_of(zr * 2, HALF), :] + rs_far[0].astype(jnp.float32)
    ).astype(jnp.bfloat16)
    red[RS_FL].wait_recv()
    rs_snd[1] = (
        p_own[rows_of(zlft * 2 + 1, HALF), :] + rs_far[1].astype(jnp.float32)
    ).astype(jnp.bfloat16)
    red[RS_SR].start()
    red[RS_SL].start()

    ig[Y_FU].wait_recv()
    y_snd[0] = (
        g[rows_of(yu * 2, SUB), :].astype(jnp.float32) + y_far[0].astype(jnp.float32)
    ).astype(jnp.bfloat16)
    ig[Y_FD].wait_recv()
    y_snd[1] = (
        g[rows_of(yd * 2 + 1, SUB), :].astype(jnp.float32) + y_far[1].astype(jnp.float32)
    ).astype(jnp.bfloat16)
    ig[Y_SU].start()
    ig[Y_SD].start()

    for number in (Y_OU, Y_OD, Y_SU, Y_SD):
        ig[number].wait_recv()
    for h in range(2):
        tot[h] = (
            gown[h * SUB:(h + 1) * SUB, :]
            + y_own[h].astype(jnp.float32) + y_sum[h].astype(jnp.float32)
        )
    z_snd[...] = tot[1 - zl].astype(jnp.bfloat16)
    across = copy(z_snd, z_rcv, Z_PAIR, pair)
    across.start()

    for number in (RS_OR, RS_OL, RS_SR, RS_SL):
        red[number].wait_recv()
    parts = jnp.zeros((OWN, 128), jnp.float32)
    for k in range(COLS // 128):
        at = slice(k * 128, (k + 1) * 128)
        both = []
        for h in range(2):
            both.append(
                p_own[rows_of(zh * 2 + h, HALF), at]
                + rs_own[h, :, at].astype(jnp.float32) + rs_sum[h, :, at].astype(jnp.float32)
            )
        summed = jnp.concatenate(both, axis=0)
        wg_out[:, at] = summed * ins[:, at]
        parts = parts + summed * fac[:, at]
    padded = jnp.concatenate([parts, jnp.zeros((256 - OWN, 128), jnp.float32)], axis=0)
    x_snd[...] = jnp.broadcast_to(
        jnp.sum(jnp.transpose(padded), axis=0, keepdims=True) * GRAD_FACTOR, (8, 256)
    )
    sends = [copy(x_snd, x_rcv.at[k], X_SUM + k, crosses[k]) for k in range(3)]
    for send in sends:
        send.start()

    across.wait_recv()
    ig_out[...] = (tot[zl] + z_rcv[...].astype(jnp.float32)).astype(jnp.bfloat16)

    for send in sends:
        send.wait_recv()
    total = x_snd[...] + x_rcv[0] + x_rcv[1] + x_rcv[2]
    sg_out[...] = total[0:1, 0:OWN]

    for group in (ag, red, ig):
        for item in group.values():
            item.wait_send()
    for j in range(4):
        to_peer(j).wait_send()
    across.wait_send()
    for send in sends:
        send.wait_send()


def shards(activations, out_grad, weight, step_size):
    bf16, f32 = jnp.bfloat16, jnp.float32
    hbm = pl.BlockSpec(memory_space=pltpu.HBM)
    vmem = pl.BlockSpec(memory_space=pltpu.VMEM)
    input_grad, weight_grad, step_rows = pl.pallas_call(
        kernel,
        out_shape=(
            jax.ShapeDtypeStruct((SUB, COLS), bf16),
            jax.ShapeDtypeStruct((OWN, COLS), f32),
            jax.ShapeDtypeStruct((1, OWN), f32),
        ),
        in_specs=[hbm] * 4,
        out_specs=(vmem, vmem, vmem),
        scratch_shapes=[
            pltpu.VMEM((TOKENS, COLS), bf16),
            pltpu.VMEM((TOKENS, ROWS), bf16),
            pltpu.VMEM((OWN, COLS), f32),
            pltpu.VMEM((1, ROWS), f32),
            pltpu.VMEM((ROWS, 128), f32),
            pltpu.VMEM((ROWS, TOKENS), bf16),
            pltpu.VMEM((ROWS, COLS), bf16),
            pltpu.VMEM((OWN, COLS), f32),
            pltpu.VMEM((OWN, COLS), f32),
            pltpu.VMEM((4 * OWN, COLS), f32),
            pltpu.VMEM((4 * OWN, COLS), bf16),
            pltpu.VMEM((4 * OWN, COLS), bf16),
            pltpu.VMEM((4 * OWN, COLS), bf16),
            pltpu.VMEM((2, HALF, COLS), bf16),
            pltpu.VMEM((2, HALF, COLS), bf16),
            pltpu.VMEM((2, HALF, COLS), bf16),
            pltpu.VMEM((2, HALF, COLS), bf16),
            pltpu.VMEM((TOKENS, COLS), bf16),
            pltpu.VMEM((2 * SUB, COLS), f32),
            pltpu.VMEM((2, SUB, COLS), bf16),
            pltpu.VMEM((2, SUB, COLS), bf16),
            pltpu.VMEM((2, SUB, COLS), bf16),
            pltpu.VMEM((2, SUB, COLS), bf16),
            pltpu.VMEM((2, SUB, COLS), f32),
            pltpu.VMEM((SUB, COLS), bf16),
            pltpu.VMEM((SUB, COLS), bf16),
            pltpu.VMEM((8, 256), f32),
            pltpu.VMEM((3, 8, 256), f32),
            pltpu.SemaphoreType.DMA((N_COPIES,)),
            pltpu.SemaphoreType.DMA((N_COPIES,)),
            pltpu.SemaphoreType.DMA((4,)),
        ],
        compiler_params=pltpu.CompilerParams(
            collective_id=0, has_side_effects=True, vmem_limit_bytes=60 * 1024 * 1024
        ),
        name="backward",
    )(activations, out_grad, weight[0], step_size)
    return (input_grad, weight_grad[None], step_rows)


def solution(mesh):
    split = Mesh(mesh.devices.reshape(4, 2, 4, 2, 4), ("zh", "core", "y", "zl", "x"))
    in_specs = (P(DP, "x"), P(DP, ROW), P(ROW, DP, "x"), P(ROW, None))
    out_specs = (P(DP + ROW, "x"), P(ROW, DP, "x"), P(ROW, DP))
    return jax.shard_map(
        shards, mesh=split, in_specs=in_specs, out_specs=out_specs, check_vma=False
    )
```

```python
import functools

import jax
import jax.numpy as jnp
from jax import lax
from jax.experimental import pallas as pl
from jax.experimental.pallas import tpu as pltpu
from jax.sharding import Mesh
from jax.sharding import PartitionSpec as P

MESH = pl.DeviceIdType.MESH
D = 4096
DP = ("zh", "core")
ROW = ("y", "zl")
OWN = 224
HALF = 112
COLS = 1024
ROWS = 1792
TOKENS = 1024
SUB = 128
GRAD_FACTOR = 1.0 / (7.0 * D) ** 0.5

AG_RA, AG_RB, AG_LB, AG_LA, AG_FR, AG_FL = range(6)
D_OWN, D_LEFT, D_RIGHT, D_FAR = range(6, 10)
D_P = 10
RS_FR, RS_FL, RS_OR, RS_OL, RS_SR, RS_SL = range(14, 20)
Y_FU, Y_FD, Y_OU, Y_OD, Y_SU, Y_SD = range(20, 26)
Z_PAIR = 26
X_SUM = 27
N_COPIES = 30


def rows_of(index, size):
    return pl.ds(pl.multiple_of(index * size, size), size)


def kernel(
    act_hbm, og_hbm, w_hbm, s_hbm,
    ig_out, wg_out, sg_out,
    act, og, w, s, scol, ogt, q, fac, ins,
    p_own, p_snd, p_rcv, c_buf,
    rs_far, rs_own, rs_sum, rs_snd,
    g, gown, y_far, y_own, y_sum, y_snd, tot, z_snd, z_rcv,
    x_snd, x_rcv,
    ss, rs, ls,
):
    zh = lax.axis_index("zh")
    core = lax.axis_index("core")
    y = lax.axis_index("y")
    zl = lax.axis_index("zl")
    x = lax.axis_index("x")
    zr, zlft, zf = (zh + 1) % 4, (zh + 3) % 4, (zh + 2) % 4
    right, left = {"zh": zr}, {"zh": zlft}
    other = 1 - core
    peer = {"core": other}
    yu, yd, yf = (y + 1) % 4, (y + 3) % 4, (y + 2) % 4
    up, down = {"y": yu}, {"y": yd}
    pair = {"zl": 1 - zl}
    crosses = [{"x": (x + k) % 4} for k in (1, 2, 3)]

    loads = [
        pltpu.make_async_copy(w_hbm, w, ls.at[0]),
        pltpu.make_async_copy(s_hbm, s, ls.at[1]),
        pltpu.make_async_copy(og_hbm, og, ls.at[2]),
        pltpu.make_async_copy(act_hbm, act, ls.at[3]),
    ]
    for load in loads:
        load.start()

    barrier = pltpu.get_barrier_semaphore()
    partners = [right, left, peer, up, down, pair] + crosses
    for partner in partners:
        pl.semaphore_signal(barrier, inc=1, device_id=partner, device_id_type=MESH)

    def copy(src, dst, number, device):
        return pltpu.make_async_remote_copy(
            src_ref=src, dst_ref=dst, send_sem=ss.at[number], recv_sem=rs.at[number],
            device_id=device, device_id_type=MESH,
        )

    def shard(j, c):
        return q.at[rows_of(j * 2 + c, OWN)]

    def half(j, c, h):
        return q.at[rows_of((j * 2 + c) * 2 + h, HALF)]

    loads[1].wait()
    scol[...] = jnp.transpose(jnp.broadcast_to(s[...], (128, ROWS)))
    loads[0].wait()
    own_row = (zh * 2 + core) * OWN
    own_at = pl.ds(pl.multiple_of(own_row, OWN), OWN)
    scale = scol[own_at, :]
    for k in range(COLS // 128):
        at = slice(k * 128, (k + 1) * 128)
        ratio = w[:, at] / scale
        levels = jnp.floor(jnp.clip(ratio, -8.0, 7.0) + 0.5)
        q[own_at, at] = (levels * scale).astype(jnp.bfloat16)

    pl.semaphore_wait(barrier, len(partners))

    ag = {
        AG_RA: copy(half(zh, core, 0), half(zh, core, 0), AG_RA, right),
        AG_RB: copy(half(zh, core, 1), half(zh, core, 1), AG_RB, right),
        AG_LB: copy(half(zh, core, 1), half(zh, core, 1), AG_LB, left),
        AG_LA: copy(half(zh, core, 0), half(zh, core, 0), AG_LA, left),
        AG_FR: copy(half(zlft, core, 0), half(zlft, core, 0), AG_FR, right),
        AG_FL: copy(half(zr, core, 1), half(zr, core, 1), AG_FL, left),
        D_OWN: copy(shard(zh, core), shard(zh, core), D_OWN, peer),
        D_LEFT: copy(shard(zlft, core), shard(zlft, core), D_LEFT, peer),
        D_RIGHT: copy(shard(zr, core), shard(zr, core), D_RIGHT, peer),
        D_FAR: copy(shard(zf, core), shard(zf, core), D_FAR, peer),
    }
    for number in (AG_RA, AG_LB, AG_RB, AG_LA, D_OWN):
        ag[number].start()

    for k in range(COLS // 128):
        at = slice(k * 128, (k + 1) * 128)
        ratio = w[:, at] / scale
        clipped = jnp.clip(ratio, -8.0, 7.0)
        levels = jnp.floor(clipped + 0.5)
        inside = (ratio >= -8.0) & (ratio <= 7.0)
        ins[:, at] = jnp.where(inside, 1.0, 0.0)
        fac[:, at] = jnp.where(inside, levels - ratio, clipped)

    loads[2].wait()
    for k in range(ROWS // 128):
        at = slice(k * 128, (k + 1) * 128)
        ogt[at, :] = jnp.transpose(og[:, at])
    loads[3].wait()

    def product(j, c, n):
        return jnp.dot(
            ogt[rows_of(j * 2 + c, OWN), :], act[:, n * 256:(n + 1) * 256],
            preferred_element_type=jnp.float32,
        )

    def to_peer(j):
        return copy(
            p_snd.at[rows_of(j, OWN)], p_rcv.at[rows_of(j, OWN)], D_P + j, peer
        )

    @pl.loop(0, 4)
    def _(j):
        for n in range(4):
            p_snd[rows_of(j, OWN), n * 256:(n + 1) * 256] = product(j, other, n).astype(jnp.bfloat16)

        @pl.when(j >= 1)
        def _():
            to_peer(j - 1).start()

    @pl.loop(0, 4)
    def _(j):
        for n in range(4):
            p_own[rows_of(j, OWN), n * 256:(n + 1) * 256] = product(j, core, n)

        @pl.when(j == 0)
        def _():
            to_peer(3).start()

    ag[AG_RA].wait_recv()
    ag[AG_LB].wait_recv()
    ag[AG_FR].start()
    ag[AG_FL].start()

    @pl.loop(0, 4)
    def _(j):
        to_peer(j).wait_recv()
        at = rows_of(j, OWN)
        total = p_own[at, :] + p_rcv[at, :].astype(jnp.float32)
        p_own[at, :] = total
        c_buf[at, :] = total.astype(jnp.bfloat16)

    def c_half(j, h):
        return c_buf.at[rows_of(j * 2 + h, HALF)]

    red = {
        RS_FR: copy(c_half(zf, 0), rs_far.at[0], RS_FR, right),
        RS_FL: copy(c_half(zf, 1), rs_far.at[1], RS_FL, left),
        RS_OR: copy(c_half(zr, 1), rs_own.at[1], RS_OR, right),
        RS_OL: copy(c_half(zlft, 0), rs_own.at[0], RS_OL, left),
        RS_SR: copy(rs_snd.at[0], rs_sum.at[0], RS_SR, right),
        RS_SL: copy(rs_snd.at[1], rs_sum.at[1], RS_SL, left),
    }
    for number in (RS_FR, RS_FL, RS_OR, RS_OL):
        red[number].start()

    ag[AG_RB].wait_recv()
    ag[D_LEFT].start()
    ag[AG_LA].wait_recv()
    ag[D_RIGHT].start()
    ag[AG_FR].wait_recv()
    ag[AG_FL].wait_recv()
    ag[D_FAR].start()
    for number in (D_OWN, D_LEFT, D_RIGHT, D_FAR):
        ag[number].wait_recv()

    def g_half(j, h):
        return g.at[rows_of(j * 2 + h, SUB)]

    ig = {
        Y_FU: copy(g_half(yf, 0), y_far.at[0], Y_FU, up),
        Y_FD: copy(g_half(yf, 1), y_far.at[1], Y_FD, down),
        Y_OU: copy(g_half(yu, 1), y_own.at[1], Y_OU, up),
        Y_OD: copy(g_half(yd, 0), y_own.at[0], Y_OD, down),
        Y_SU: copy(y_snd.at[0], y_sum.at[0], Y_SU, up),
        Y_SD: copy(y_snd.at[1], y_sum.at[1], Y_SD, down),
    }

    def block(t, n):
        return jnp.dot(
            og[rows_of(t, 2 * SUB), :], q[:, n * 256:(n + 1) * 256],
            preferred_element_type=jnp.float32,
        )

    @pl.loop(0, 3)
    def _(k):
        t = jnp.where(k == 0, yf, jnp.where(k == 1, yu, yd))
        for n in range(4):
            g[rows_of(t, 2 * SUB), n * 256:(n + 1) * 256] = block(t, n).astype(jnp.bfloat16)

        @pl.when(k == 0)
        def _():
            ig[Y_FU].start()
            ig[Y_FD].start()

    ig[Y_OU].start()
    ig[Y_OD].start()
    for n in range(4):
        gown[:, n * 256:(n + 1) * 256] = block(y, n)

    red[RS_FR].wait_recv()
    rs_snd[0] = (
        p_own[rows_of(zr * 2, HALF), :] + rs_far[0].astype(jnp.float32)
    ).astype(jnp.bfloat16)
    red[RS_FL].wait_recv()
    rs_snd[1] = (
        p_own[rows_of(zlft * 2 + 1, HALF), :] + rs_far[1].astype(jnp.float32)
    ).astype(jnp.bfloat16)
    red[RS_SR].start()
    red[RS_SL].start()

    ig[Y_FU].wait_recv()
    y_snd[0] = (
        g[rows_of(yu * 2, SUB), :].astype(jnp.float32) + y_far[0].astype(jnp.float32)
    ).astype(jnp.bfloat16)
    ig[Y_FD].wait_recv()
    y_snd[1] = (
        g[rows_of(yd * 2 + 1, SUB), :].astype(jnp.float32) + y_far[1].astype(jnp.float32)
    ).astype(jnp.bfloat16)
    ig[Y_SU].start()
    ig[Y_SD].start()

    for number in (Y_OU, Y_OD, Y_SU, Y_SD):
        ig[number].wait_recv()
    for h in range(2):
        tot[h] = (
            gown[h * SUB:(h + 1) * SUB, :]
            + y_own[h].astype(jnp.float32) + y_sum[h].astype(jnp.float32)
        )
    z_snd[...] = tot[1 - zl].astype(jnp.bfloat16)
    across = copy(z_snd, z_rcv, Z_PAIR, pair)
    across.start()

    for number in (RS_OR, RS_OL, RS_SR, RS_SL):
        red[number].wait_recv()
    parts = jnp.zeros((OWN, 128), jnp.float32)
    for k in range(COLS // 128):
        at = slice(k * 128, (k + 1) * 128)
        both = []
        for h in range(2):
            both.append(
                p_own[rows_of(zh * 2 + h, HALF), at]
                + rs_own[h, :, at].astype(jnp.float32) + rs_sum[h, :, at].astype(jnp.float32)
            )
        summed = jnp.concatenate(both, axis=0)
        wg_out[:, at] = summed * ins[:, at]
        parts = parts + summed * fac[:, at]
    padded = jnp.concatenate([parts, jnp.zeros((256 - OWN, 128), jnp.float32)], axis=0)
    x_snd[...] = jnp.broadcast_to(
        jnp.sum(jnp.transpose(padded), axis=0, keepdims=True) * GRAD_FACTOR, (8, 256)
    )
    sends = [copy(x_snd, x_rcv.at[k], X_SUM + k, crosses[k]) for k in range(3)]
    for send in sends:
        send.start()

    across.wait_recv()
    ig_out[...] = (tot[zl] + z_rcv[...].astype(jnp.float32)).astype(jnp.bfloat16)

    for send in sends:
        send.wait_recv()
    total = x_snd[...] + x_rcv[0] + x_rcv[1] + x_rcv[2]
    sg_out[...] = total[0:1, 0:OWN]

    for group in (ag, red, ig):
        for item in group.values():
            item.wait_send()
    for j in range(4):
        to_peer(j).wait_send()
    across.wait_send()
    for send in sends:
        send.wait_send()


def store(ig_ref, wg_ref, sg_ref, ig_hbm, wg_hbm, sg_hbm, sems):
    moves = [
        pltpu.make_async_copy(wg_ref, wg_hbm, sems.at[0]),
        pltpu.make_async_copy(ig_ref, ig_hbm, sems.at[1]),
        pltpu.make_async_copy(sg_ref, sg_hbm, sems.at[2]),
    ]
    for move in moves:
        move.start()
    for move in moves:
        move.wait()


def shards(activations, out_grad, weight, step_size):
    bf16, f32 = jnp.bfloat16, jnp.float32
    hbm = pl.BlockSpec(memory_space=pltpu.HBM)
    vmem = pl.BlockSpec(memory_space=pltpu.VMEM)
    input_grad, weight_grad, step_rows = pl.pallas_call(
        kernel,
        out_shape=(
            pltpu.VMEM((SUB, COLS), bf16),
            pltpu.VMEM((OWN, COLS), f32),
            pltpu.VMEM((1, OWN), f32),
        ),
        in_specs=[hbm] * 4,
        out_specs=(vmem, vmem, vmem),
        scratch_shapes=[
            pltpu.VMEM((TOKENS, COLS), bf16),
            pltpu.VMEM((TOKENS, ROWS), bf16),
            pltpu.VMEM((OWN, COLS), f32),
            pltpu.VMEM((1, ROWS), f32),
            pltpu.VMEM((ROWS, 128), f32),
            pltpu.VMEM((ROWS, TOKENS), bf16),
            pltpu.VMEM((ROWS, COLS), bf16),
            pltpu.VMEM((OWN, COLS), f32),
            pltpu.VMEM((OWN, COLS), f32),
            pltpu.VMEM((4 * OWN, COLS), f32),
            pltpu.VMEM((4 * OWN, COLS), bf16),
            pltpu.VMEM((4 * OWN, COLS), bf16),
            pltpu.VMEM((4 * OWN, COLS), bf16),
            pltpu.VMEM((2, HALF, COLS), bf16),
            pltpu.VMEM((2, HALF, COLS), bf16),
            pltpu.VMEM((2, HALF, COLS), bf16),
            pltpu.VMEM((2, HALF, COLS), bf16),
            pltpu.VMEM((TOKENS, COLS), bf16),
            pltpu.VMEM((2 * SUB, COLS), f32),
            pltpu.VMEM((2, SUB, COLS), bf16),
            pltpu.VMEM((2, SUB, COLS), bf16),
            pltpu.VMEM((2, SUB, COLS), bf16),
            pltpu.VMEM((2, SUB, COLS), bf16),
            pltpu.VMEM((2, SUB, COLS), f32),
            pltpu.VMEM((SUB, COLS), bf16),
            pltpu.VMEM((SUB, COLS), bf16),
            pltpu.VMEM((8, 256), f32),
            pltpu.VMEM((3, 8, 256), f32),
            pltpu.SemaphoreType.DMA((N_COPIES,)),
            pltpu.SemaphoreType.DMA((N_COPIES,)),
            pltpu.SemaphoreType.DMA((4,)),
        ],
        compiler_params=pltpu.CompilerParams(
            collective_id=0, has_side_effects=True, vmem_limit_bytes=60*1024*1024
        ),
        name="backward",
    )(activations, out_grad, weight[0], step_size)
    outs = pl.pallas_call(
        store,
        out_shape=(
            jax.ShapeDtypeStruct((SUB, COLS), bf16),
            jax.ShapeDtypeStruct((OWN, COLS), f32),
            jax.ShapeDtypeStruct((1, OWN), f32),
        ),
        in_specs=[vmem] * 3,
        out_specs=(hbm,) * 3,
        scratch_shapes=[pltpu.SemaphoreType.DMA((3,))],
        compiler_params=pltpu.CompilerParams(vmem_limit_bytes=4 * 1024 * 1024),
        name="store",
    )(input_grad, weight_grad, step_rows)
    return (outs[0], outs[1][None], outs[2])


def solution(mesh):
    split = Mesh(mesh.devices.reshape(4, 2, 4, 2, 4), ("zh", "core", "y", "zl", "x"))
    in_specs = (P(DP, "x"), P(DP, ROW), P(ROW, DP, "x"), P(ROW, None))
    out_specs = (P(DP + ROW, "x"), P(ROW, DP, "x"), P(ROW, DP))
    return jax.shard_map(
        shards, mesh=split, in_specs=in_specs, out_specs=out_specs, check_vma=False
    )
```

```python
import functools

import jax
import jax.numpy as jnp
from jax import lax
from jax.experimental import pallas as pl
from jax.experimental.pallas import tpu as pltpu
from jax.sharding import Mesh
from jax.sharding import PartitionSpec as P

MESH = pl.DeviceIdType.MESH
D = 4096
DP = ("zh", "core")
ROW = ("y", "zl")
OWN = 224
HALF = 112
COLS = 1024
ROWS = 1792
TOKENS = 1024
SUB = 128
GRAD_FACTOR = 1.0 / (7.0 * D) ** 0.5

AG_RA, AG_RB, AG_LB, AG_LA, AG_FR, AG_FL = range(6)
D_OWN, D_LEFT, D_RIGHT, D_FAR = range(6, 10)
D_P = 10
RS_FAR, RS_ONE, RS_SUM = 14, 16, 18
Y_FP, Y_FM, Y_OP, Y_OM, Y_SP, Y_SM = range(20, 26)
Z_PAIR = 26
X_SUM = 27
T_PAIR = 30
T_X = 31
N_COPIES = 34


def rows_of(index, size):
    return pl.ds(pl.multiple_of(index * size, size), size)


def kernel(
    act_hbm, og_hbm, w_hbm, s_hbm,
    ig_out, wg_out, sg_out,
    act, og, w, s, scol, ogt, ogt_pair, q, fac, ins,
    p_own, p_snd, p_rcv, c_buf,
    rs_far, rs_one, rs_sum, rs_snd, parts,
    g, gown, y_far, y_own, y_sum, y_snd, mine, z_snd, z_rcv,
    x_snd, x_rcv,
    ss, rs, ls,
):
    zh = lax.axis_index("zh")
    core = lax.axis_index("core")
    y = lax.axis_index("y")
    zl = lax.axis_index("zl")
    x = lax.axis_index("x")
    zr, zlft, zf = (zh + 1) % 4, (zh + 3) % 4, (zh + 2) % 4
    right, left = {"zh": zr}, {"zh": zlft}
    zs = (zh + 3 + 2 * zl) % 4
    zo = (zh + 1 + 2 * zl) % 4
    chain = {"zh": zs}
    beside = {"zh": zs, "zl": 1 - zl}
    other = 1 - core
    peer = {"core": other}
    yf = (y + 2) % 4
    pair = {"zl": 1 - zl}
    crosses = [{"x": (x + k) % 4} for k in (1, 2, 3)]
    hp = 1 - zl
    yp = (y + 1 + 2 * hp) % 4
    ym = (y + 3 + 2 * hp) % 4
    way_p, way_m = {"y": yp}, {"y": ym}

    loads = [
        pltpu.make_async_copy(s_hbm, s, ls.at[0]),
        pltpu.make_async_copy(w_hbm, w, ls.at[1]),
        pltpu.make_async_copy(og_hbm, og, ls.at[2]),
        pltpu.make_async_copy(act_hbm, act, ls.at[3]),
    ]
    for load in loads:
        load.start()

    barrier = pltpu.get_barrier_semaphore()
    partners = [right, left, beside, peer, way_p, way_m, pair] + crosses
    for partner in partners:
        pl.semaphore_signal(barrier, inc=1, device_id=partner, device_id_type=MESH)

    def copy(src, dst, number, device):
        return pltpu.make_async_remote_copy(
            src_ref=src, dst_ref=dst, send_sem=ss.at[number], recv_sem=rs.at[number],
            device_id=device, device_id_type=MESH,
        )

    def shard(j, c):
        return q.at[rows_of(j * 2 + c, OWN)]

    def half(j, c, h):
        return q.at[rows_of((j * 2 + c) * 2 + h, HALF)]

    loads[0].wait()
    scol[...] = jnp.transpose(jnp.broadcast_to(s[...], (128, ROWS)))
    loads[1].wait()
    own_at = rows_of(zh * 2 + core, OWN)
    scale = scol[own_at, :]
    for k in range(COLS // 128):
        at = slice(k * 128, (k + 1) * 128)
        ratio = w[:, at] / scale
        levels = jnp.floor(jnp.clip(ratio, -8.0, 7.0) + 0.5)
        q[own_at, at] = (levels * scale).astype(jnp.bfloat16)

    pl.semaphore_wait(barrier, len(partners))

    ag = {
        AG_RA: copy(half(zh, core, 0), half(zh, core, 0), AG_RA, right),
        AG_RB: copy(half(zh, core, 1), half(zh, core, 1), AG_RB, right),
        AG_LB: copy(half(zh, core, 1), half(zh, core, 1), AG_LB, left),
        AG_LA: copy(half(zh, core, 0), half(zh, core, 0), AG_LA, left),
        AG_FR: copy(half(zlft, core, 0), half(zlft, core, 0), AG_FR, right),
        AG_FL: copy(half(zr, core, 1), half(zr, core, 1), AG_FL, left),
        D_OWN: copy(shard(zh, core), shard(zh, core), D_OWN, peer),
        D_LEFT: copy(shard(zlft, core), shard(zlft, core), D_LEFT, peer),
        D_RIGHT: copy(shard(zr, core), shard(zr, core), D_RIGHT, peer),
        D_FAR: copy(shard(zf, core), shard(zf, core), D_FAR, peer),
    }
    for number in (AG_RA, AG_LB, AG_RB, AG_LA, D_OWN):
        ag[number].start()

    loads[2].wait()
    for k in range(ROWS // 128):
        at = slice(k * 128, (k + 1) * 128)
        ogt[at, :] = jnp.transpose(og[:, at])

    for k in range(COLS // 128):
        at = slice(k * 128, (k + 1) * 128)
        ratio = w[:, at] / scale
        clipped = jnp.clip(ratio, -8.0, 7.0)
        levels = jnp.floor(clipped + 0.5)
        inside = (ratio >= -8.0) & (ratio <= 7.0)
        ins[:, at] = jnp.where(inside, 1.0, 0.0)
        fac[:, at] = jnp.where(inside, levels - ratio, clipped)

    quarter = ogt_pair.at[rows_of(x, HALF)]
    turned = copy(ogt.at[rows_of(zo * 4 + x, HALF)], quarter, T_PAIR, pair)
    turned.start()
    loads[3].wait()

    def product(rows, at, c, n):
        return jnp.dot(
            rows[rows_of(at * 2 + c, OWN), :], act[:, n * 256:(n + 1) * 256],
            preferred_element_type=jnp.float32,
        )

    def to_peer(b):
        return copy(
            p_snd.at[rows_of(b, OWN)], p_rcv.at[rows_of(b, OWN)], D_P + b, peer
        )

    @pl.loop(0, 3)
    def _(b):
        dest = jnp.where(b == 0, zf, jnp.where(b == 1, zs, zh))
        for n in range(4):
            at = slice(n * 256, (n + 1) * 256)
            p_snd[rows_of(b, OWN), at] = product(ogt, dest, other, n).astype(jnp.bfloat16)
        for n in range(4):
            at = slice(n * 256, (n + 1) * 256)
            p_own[rows_of(b, OWN), at] = product(ogt, dest, core, n)
        to_peer(b).start()

    turned.wait_recv()
    shares = [copy(quarter, quarter, T_X + k, crosses[k]) for k in range(3)]
    for share in shares:
        share.start()

    ag[AG_RA].wait_recv()
    ag[AG_LB].wait_recv()
    ag[AG_FR].start()
    ag[AG_FL].start()

    for share in shares:
        share.wait_recv()
    for n in range(4):
        at = slice(n * 256, (n + 1) * 256)
        p_snd[3 * OWN:, at] = product(ogt_pair, 0, other, n).astype(jnp.bfloat16)
    for n in range(4):
        at = slice(n * 256, (n + 1) * 256)
        p_own[3 * OWN:, at] = product(ogt_pair, 0, core, n)
    to_peer(3).start()

    @pl.loop(0, 4)
    def _(b):
        to_peer(b).wait_recv()
        at = rows_of(b, OWN)
        total = p_own[at, :] + p_rcv[at, :].astype(jnp.float32)
        p_own[at, :] = total
        c_buf[at, :] = total.astype(jnp.bfloat16)

    def c_half(b, h):
        return c_buf.at[(2 * b + h) * HALF:(2 * b + h + 1) * HALF]

    far = [copy(c_half(0, h), rs_far.at[h], RS_FAR + h, chain) for h in range(2)]
    one = [copy(c_half(3, h), rs_one.at[h], RS_ONE + h, beside) for h in range(2)]
    whole = [copy(rs_snd.at[h], rs_sum.at[h], RS_SUM + h, chain) for h in range(2)]

    ag[AG_RB].wait_recv()
    ag[D_LEFT].start()
    ag[AG_LA].wait_recv()
    ag[D_RIGHT].start()
    ag[AG_FR].wait_send()
    ag[AG_FL].wait_send()
    for item in far + one:
        item.start()
    ag[AG_FR].wait_recv()
    ag[AG_FL].wait_recv()
    ag[D_FAR].start()
    for number in (D_OWN, D_LEFT, D_RIGHT, D_FAR):
        ag[number].wait_recv()

    def g_half(j, h):
        return g.at[rows_of(j * 2 + h, SUB)]

    ig = {
        Y_FP: copy(g_half(yf, hp), y_far.at[0], Y_FP, way_p),
        Y_FM: copy(g_half(yf, zl), y_far.at[1], Y_FM, way_m),
        Y_OP: copy(g_half(ym, hp), y_own.at[0], Y_OP, way_m),
        Y_OM: copy(g_half(yp, zl), y_own.at[1], Y_OM, way_p),
        Y_SP: copy(y_snd.at[0], y_sum.at[0], Y_SP, way_p),
        Y_SM: copy(y_snd.at[1], y_sum.at[1], Y_SM, way_m),
    }

    def block(t, n):
        return jnp.dot(
            og[rows_of(t, 2 * SUB), :], q[:, n * 256:(n + 1) * 256],
            preferred_element_type=jnp.float32,
        )

    @pl.loop(0, 3)
    def _(k):
        t = jnp.where(k == 0, yf, jnp.where(k == 1, ym, yp))
        for n in range(4):
            g[rows_of(t, 2 * SUB), n * 256:(n + 1) * 256] = block(t, n).astype(jnp.bfloat16)

        @pl.when(k == 0)
        def _():
            ig[Y_FP].start()
            ig[Y_FM].start()

        @pl.when(k == 1)
        def _():
            ig[Y_OP].start()

    for n in range(4):
        gown[:, n * 256:(n + 1) * 256] = block(y, n)

    def middle(h):
        far[h].wait_recv()
        rs_snd[h] = (
            p_own[OWN + h * HALF:OWN + (h + 1) * HALF, :] + rs_far[h].astype(jnp.float32)
        ).astype(jnp.bfloat16)
        whole[h].start()

    middle(0)
    ig[Y_FP].wait_recv()
    y_snd[0] = (
        g[rows_of(yp * 2 + hp, SUB), :].astype(jnp.float32) + y_far[0].astype(jnp.float32)
    ).astype(jnp.bfloat16)
    ig[Y_SP].start()
    ig[Y_OM].start()
    ig[Y_FM].wait_recv()
    y_snd[1] = (
        g[rows_of(ym * 2 + zl, SUB), :].astype(jnp.float32) + y_far[1].astype(jnp.float32)
    ).astype(jnp.bfloat16)
    ig[Y_SM].start()
    middle(1)

    ig[Y_OP].wait_recv()
    ig[Y_SP].wait_recv()
    z_snd[...] = (
        gown[rows_of(hp, SUB), :] + y_own[0].astype(jnp.float32) + y_sum[0].astype(jnp.float32)
    ).astype(jnp.bfloat16)
    across = copy(z_snd, z_rcv, Z_PAIR, pair)
    across.start()
    ig[Y_OM].wait_recv()
    ig[Y_SM].wait_recv()
    mine[...] = (
        gown[rows_of(zl, SUB), :] + y_own[1].astype(jnp.float32) + y_sum[1].astype(jnp.float32)
    )

    def finish(h):
        one[h].wait_recv()
        whole[h].wait_recv()
        rows = slice(h * HALF, (h + 1) * HALF)
        part = jnp.zeros((HALF, 128), jnp.float32)
        for k in range(COLS // 128):
            at = slice(k * 128, (k + 1) * 128)
            summed = (
                p_own[2 * OWN + h * HALF:2 * OWN + (h + 1) * HALF, at]
                + rs_one[h, :, at].astype(jnp.float32) + rs_sum[h, :, at].astype(jnp.float32)
            )
            wg_out[rows, at] = summed * ins[rows, at]
            part = part + summed * fac[rows, at]
        parts[rows, :] = part

    parts[OWN:, :] = jnp.zeros((256 - OWN, 128), jnp.float32)
    finish(0)
    across.wait_recv()
    ig_out[...] = (mine[...] + z_rcv[...].astype(jnp.float32)).astype(jnp.bfloat16)
    finish(1)
    x_snd[...] = jnp.broadcast_to(
        jnp.sum(jnp.transpose(parts[...]), axis=0, keepdims=True) * GRAD_FACTOR, (8, 256)
    )
    sends = [copy(x_snd, x_rcv.at[k], X_SUM + k, crosses[k]) for k in range(3)]
    for send in sends:
        send.start()

    for number in ag:
        if number not in (AG_FR, AG_FL):
            ag[number].wait_send()
    for item in list(ig.values()) + far + one + whole + shares + [turned, across]:
        item.wait_send()
    for b in range(4):
        to_peer(b).wait_send()

    for send in sends:
        send.wait_recv()
    total = x_snd[...] + x_rcv[0] + x_rcv[1] + x_rcv[2]
    sg_out[...] = total[0:1, 0:OWN]
    for send in sends:
        send.wait_send()


def store(ig_ref, wg_ref, sg_ref, ig_hbm, wg_hbm, sg_hbm, sems):
    moves = [
        pltpu.make_async_copy(wg_ref, wg_hbm, sems.at[0]),
        pltpu.make_async_copy(ig_ref, ig_hbm, sems.at[1]),
        pltpu.make_async_copy(sg_ref, sg_hbm, sems.at[2]),
    ]
    for move in moves:
        move.start()
    for move in moves:
        move.wait()


def shards(activations, out_grad, weight, step_size):
    bf16, f32 = jnp.bfloat16, jnp.float32
    hbm = pl.BlockSpec(memory_space=pltpu.HBM)
    vmem = pl.BlockSpec(memory_space=pltpu.VMEM)
    input_grad, weight_grad, step_rows = pl.pallas_call(
        kernel,
        out_shape=(
            pltpu.VMEM((SUB, COLS), bf16),
            pltpu.VMEM((OWN, COLS), f32),
            pltpu.VMEM((1, OWN), f32),
        ),
        in_specs=[hbm] * 4,
        out_specs=(vmem, vmem, vmem),
        scratch_shapes=[
            pltpu.VMEM((TOKENS, COLS), bf16),
            pltpu.VMEM((TOKENS, ROWS), bf16),
            pltpu.VMEM((OWN, COLS), f32),
            pltpu.VMEM((1, ROWS), f32),
            pltpu.VMEM((ROWS, 128), f32),
            pltpu.VMEM((ROWS, TOKENS), bf16),
            pltpu.VMEM((2 * OWN, TOKENS), bf16),
            pltpu.VMEM((ROWS, COLS), bf16),
            pltpu.VMEM((OWN, COLS), f32),
            pltpu.VMEM((OWN, COLS), f32),
            pltpu.VMEM((4 * OWN, COLS), f32),
            pltpu.VMEM((4 * OWN, COLS), bf16),
            pltpu.VMEM((4 * OWN, COLS), bf16),
            pltpu.VMEM((4 * OWN, COLS), bf16),
            pltpu.VMEM((2, HALF, COLS), bf16),
            pltpu.VMEM((2, HALF, COLS), bf16),
            pltpu.VMEM((2, HALF, COLS), bf16),
            pltpu.VMEM((2, HALF, COLS), bf16),
            pltpu.VMEM((256, 128), f32),
            pltpu.VMEM((TOKENS, COLS), bf16),
            pltpu.VMEM((2 * SUB, COLS), f32),
            pltpu.VMEM((2, SUB, COLS), bf16),
            pltpu.VMEM((2, SUB, COLS), bf16),
            pltpu.VMEM((2, SUB, COLS), bf16),
            pltpu.VMEM((2, SUB, COLS), bf16),
            pltpu.VMEM((SUB, COLS), f32),
            pltpu.VMEM((SUB, COLS), bf16),
            pltpu.VMEM((SUB, COLS), bf16),
            pltpu.VMEM((8, 256), f32),
            pltpu.VMEM((3, 8, 256), f32),
            pltpu.SemaphoreType.DMA((N_COPIES,)),
            pltpu.SemaphoreType.DMA((N_COPIES,)),
            pltpu.SemaphoreType.DMA((4,)),
        ],
        compiler_params=pltpu.CompilerParams(
            collective_id=0, has_side_effects=True, vmem_limit_bytes=60*1024*1024
        ),
        name="backward",
    )(activations, out_grad, weight[0], step_size)
    outs = pl.pallas_call(
        store,
        out_shape=(
            jax.ShapeDtypeStruct((SUB, COLS), bf16),
            jax.ShapeDtypeStruct((OWN, COLS), f32),
            jax.ShapeDtypeStruct((1, OWN), f32),
        ),
        in_specs=[vmem] * 3,
        out_specs=(hbm,) * 3,
        scratch_shapes=[pltpu.SemaphoreType.DMA((3,))],
        compiler_params=pltpu.CompilerParams(vmem_limit_bytes=4 * 1024 * 1024),
        name="store",
    )(input_grad, weight_grad, step_rows)
    return (outs[0], outs[1][None], outs[2])


def solution(mesh):
    split = Mesh(mesh.devices.reshape(4, 2, 4, 2, 4), ("zh", "core", "y", "zl", "x"))
    in_specs = (P(DP, "x"), P(DP, ROW), P(ROW, DP, "x"), P(ROW, None))
    out_specs = (P(DP + ROW, "x"), P(ROW, DP, "x"), P(ROW, DP))
    return jax.shard_map(
        shards, mesh=split, in_specs=in_specs, out_specs=out_specs, check_vma=False
    )
```

```python
import functools

import jax
import jax.numpy as jnp
from jax import lax
from jax.experimental import pallas as pl
from jax.experimental.pallas import tpu as pltpu
from jax.sharding import Mesh
from jax.sharding import PartitionSpec as P

MESH = pl.DeviceIdType.MESH
D = 4096
DP = ("zh", "core")
ROW = ("y", "zl")
OWN = 224
HALF = 112
COLS = 1024
ROWS = 1792
TOKENS = 1024
SUB = 128
GRAD_FACTOR = 1.0 / (7.0 * D) ** 0.5

AG_OWN, AG_FWD, AG_ONE = 0, 2, 4
D_OWN, D_NEAR, D_FAR, D_BESIDE = range(6, 10)
D_P = 10
RS_FAR, RS_ONE, RS_SUM = 14, 16, 18
Y_FP, Y_FM, Y_OP, Y_OM, Y_SP, Y_SM = range(20, 26)
Z_PAIR = 26
X_SUM = 27
T_PAIR = 30
T_X = 31
N_COPIES = 34


def rows_of(index, size):
    return pl.ds(pl.multiple_of(index * size, size), size)


def kernel(
    act_hbm, og_hbm, w_hbm, s_hbm,
    ig_out, wg_out, sg_out,
    act, og, w, s, scol, ogt, ogt_pair, q, fac, ins,
    p_own, p_snd, p_rcv, c_buf,
    rs_far, rs_one, rs_sum, rs_snd, parts,
    g, gown, y_far, y_own, y_sum, y_snd, mine, z_snd, z_rcv,
    x_snd, x_rcv,
    ss, rs, ls,
):
    zh = lax.axis_index("zh")
    core = lax.axis_index("core")
    y = lax.axis_index("y")
    zl = lax.axis_index("zl")
    x = lax.axis_index("x")
    zf = (zh + 2) % 4
    zs = (zh + 3 + 2 * zl) % 4
    zo = (zh + 1 + 2 * zl) % 4
    chain, back = {"zh": zs}, {"zh": zo}
    beside = {"zh": zs, "zl": 1 - zl}
    other = 1 - core
    peer = {"core": other}
    yf = (y + 2) % 4
    pair = {"zl": 1 - zl}
    crosses = [{"x": (x + k) % 4} for k in (1, 2, 3)]
    hp = 1 - zl
    yp = (y + 1 + 2 * hp) % 4
    ym = (y + 3 + 2 * hp) % 4
    way_p, way_m = {"y": yp}, {"y": ym}

    loads = [
        pltpu.make_async_copy(s_hbm, s, ls.at[0]),
        pltpu.make_async_copy(w_hbm, w, ls.at[1]),
        pltpu.make_async_copy(og_hbm, og, ls.at[2]),
        pltpu.make_async_copy(act_hbm, act, ls.at[3]),
    ]
    loads[0].start()
    loads[1].start()

    barrier = pltpu.get_barrier_semaphore()
    partners = [chain, back, beside, peer, way_p, way_m, pair] + crosses
    for partner in partners:
        pl.semaphore_signal(barrier, inc=1, device_id=partner, device_id_type=MESH)

    def copy(src, dst, number, device):
        return pltpu.make_async_remote_copy(
            src_ref=src, dst_ref=dst, send_sem=ss.at[number], recv_sem=rs.at[number],
            device_id=device, device_id_type=MESH,
        )

    def shard(j):
        return q.at[rows_of(j * 2 + core, OWN)]

    def half(j, h):
        return q.at[rows_of((j * 2 + core) * 2 + h, HALF)]

    loads[0].wait()
    loads[2].start()
    loads[3].start()
    scol[...] = jnp.transpose(jnp.broadcast_to(s[...], (128, ROWS)))
    loads[1].wait()
    own_at = rows_of(zh * 2 + core, OWN)
    scale = scol[own_at, :]
    for k in range(COLS // 128):
        at = slice(k * 128, (k + 1) * 128)
        ratio = w[:, at] / scale
        levels = jnp.floor(jnp.clip(ratio, -8.0, 7.0) + 0.5)
        q[own_at, at] = (levels * scale).astype(jnp.bfloat16)

    pl.semaphore_wait(barrier, len(partners))

    own = [copy(half(zh, h), half(zh, h), AG_OWN + h, back) for h in range(2)]
    fwd = [copy(half(zs, h), half(zs, h), AG_FWD + h, back) for h in range(2)]
    aside = [copy(half(zh, h), half(zf, h), AG_ONE + h, beside) for h in range(2)]
    swap = {
        D_OWN: copy(shard(zh), shard(zh), D_OWN, peer),
        D_NEAR: copy(shard(zs), shard(zs), D_NEAR, peer),
        D_FAR: copy(shard(zf), shard(zf), D_FAR, peer),
        D_BESIDE: copy(shard(zo), shard(zo), D_BESIDE, peer),
    }
    own[0].start()
    aside[0].start()
    aside[1].start()
    swap[D_OWN].start()

    loads[2].wait()
    for k in range(ROWS // 128):
        at = slice(k * 128, (k + 1) * 128)
        ogt[at, :] = jnp.transpose(og[:, at])

    quarter = ogt_pair.at[rows_of(x, HALF)]
    turned = copy(ogt.at[rows_of(zo * 4 + x, HALF)], quarter, T_PAIR, pair)
    turned.start()
    own[1].start()

    for k in range(COLS // 128):
        at = slice(k * 128, (k + 1) * 128)
        ratio = w[:, at] / scale
        clipped = jnp.clip(ratio, -8.0, 7.0)
        levels = jnp.floor(clipped + 0.5)
        inside = (ratio >= -8.0) & (ratio <= 7.0)
        ins[:, at] = jnp.where(inside, 1.0, 0.0)
        fac[:, at] = jnp.where(inside, levels - ratio, clipped)

    loads[3].wait()

    def product(at, c, n):
        return jnp.dot(
            ogt[rows_of(at * 2 + c, OWN), :], act[:, n * 256:(n + 1) * 256],
            preferred_element_type=jnp.float32,
        )

    def to_peer(b):
        return copy(
            p_snd.at[rows_of(b, OWN)], p_rcv.at[rows_of(b, OWN)], D_P + b, peer
        )

    @pl.loop(0, 3)
    def _(b):
        dest = jnp.where(b == 0, zf, jnp.where(b == 1, zs, zh))
        for n in range(4):
            at = slice(n * 256, (n + 1) * 256)
            p_snd[rows_of(b, OWN), at] = product(dest, other, n).astype(jnp.bfloat16)
        for n in range(4):
            at = slice(n * 256, (n + 1) * 256)
            p_own[rows_of(b, OWN), at] = product(dest, core, n)
        to_peer(b).start()

    def chip_sum(b):
        to_peer(b).wait_recv()
        at = rows_of(b, OWN)
        total = p_own[at, :] + p_rcv[at, :].astype(jnp.float32)
        p_own[at, :] = total
        c_buf[at, :] = total.astype(jnp.bfloat16)

    own[0].wait_recv()
    fwd[0].start()

    @pl.loop(0, 3)
    def _(b):
        chip_sum(b)

    def c_half(b, h):
        return c_buf.at[(2 * b + h) * HALF:(2 * b + h + 1) * HALF]

    far = [copy(c_half(0, h), rs_far.at[h], RS_FAR + h, chain) for h in range(2)]
    one = [copy(c_half(3, h), rs_one.at[h], RS_ONE + h, beside) for h in range(2)]
    whole = [copy(rs_snd.at[h], rs_sum.at[h], RS_SUM + h, chain) for h in range(2)]

    for item in far:
        item.start()

    turned.wait_recv()
    shares = [copy(quarter, quarter, T_X + k, crosses[k]) for k in range(3)]
    for share in shares:
        share.start()
    own[1].wait_recv()
    fwd[1].start()
    swap[D_NEAR].start()

    for share in shares:
        share.wait_recv()
    turned.wait_send()
    ogt[rows_of(zo, 2 * OWN), :] = ogt_pair[...]
    for n in range(4):
        at = slice(n * 256, (n + 1) * 256)
        p_snd[3 * OWN:, at] = product(zo, other, n).astype(jnp.bfloat16)
    for n in range(4):
        at = slice(n * 256, (n + 1) * 256)
        p_own[3 * OWN:, at] = product(zo, core, n)
    to_peer(3).start()
    for k in range(ROWS // 128):
        at = slice(k * 128, (k + 1) * 128)
        og[:, at] = jnp.transpose(ogt[at, :])
    chip_sum(3)

    one[0].start()
    for item in aside:
        item.wait_recv()
    swap[D_BESIDE].start()
    fwd[0].wait_recv()
    fwd[1].wait_recv()
    swap[D_FAR].start()
    for item in swap.values():
        item.wait_recv()

    def g_half(j, h):
        return g.at[rows_of(j * 2 + h, SUB)]

    ig = {
        Y_FP: copy(g_half(yf, hp), y_far.at[0], Y_FP, way_p),
        Y_FM: copy(g_half(yf, zl), y_far.at[1], Y_FM, way_m),
        Y_OP: copy(g_half(ym, hp), y_own.at[0], Y_OP, way_m),
        Y_OM: copy(g_half(yp, zl), y_own.at[1], Y_OM, way_p),
        Y_SP: copy(y_snd.at[0], y_sum.at[0], Y_SP, way_p),
        Y_SM: copy(y_snd.at[1], y_sum.at[1], Y_SM, way_m),
    }

    def block(t, n):
        return jnp.dot(
            og[rows_of(t, 2 * SUB), :], q[:, n * 256:(n + 1) * 256],
            preferred_element_type=jnp.float32,
        )

    @pl.loop(0, 3)
    def _(k):
        t = jnp.where(k == 0, yf, jnp.where(k == 1, ym, yp))
        for n in range(4):
            g[rows_of(t, 2 * SUB), n * 256:(n + 1) * 256] = block(t, n).astype(jnp.bfloat16)

        @pl.when(k == 0)
        def _():
            ig[Y_FP].start()
            ig[Y_FM].start()

        @pl.when(k == 1)
        def _():
            ig[Y_OP].start()

    for n in range(4):
        gown[:, n * 256:(n + 1) * 256] = block(y, n)

    def middle(h):
        far[h].wait_recv()
        rs_snd[h] = (
            p_own[OWN + h * HALF:OWN + (h + 1) * HALF, :] + rs_far[h].astype(jnp.float32)
        ).astype(jnp.bfloat16)
        whole[h].start()

    middle(0)
    ig[Y_FP].wait_recv()
    y_snd[0] = (
        g[rows_of(yp * 2 + hp, SUB), :].astype(jnp.float32) + y_far[0].astype(jnp.float32)
    ).astype(jnp.bfloat16)
    ig[Y_SP].start()
    ig[Y_OM].start()

    ig[Y_FM].wait_recv()
    y_snd[1] = (
        g[rows_of(ym * 2 + zl, SUB), :].astype(jnp.float32) + y_far[1].astype(jnp.float32)
    ).astype(jnp.bfloat16)
    ig[Y_SM].start()
    middle(1)
    one[1].start()

    ig[Y_OP].wait_recv()
    ig[Y_SP].wait_recv()
    z_snd[...] = (
        gown[rows_of(hp, SUB), :] + y_own[0].astype(jnp.float32) + y_sum[0].astype(jnp.float32)
    ).astype(jnp.bfloat16)
    across = copy(z_snd, z_rcv, Z_PAIR, pair)
    across.start()
    ig[Y_OM].wait_recv()
    ig[Y_SM].wait_recv()
    mine[...] = (
        gown[rows_of(zl, SUB), :] + y_own[1].astype(jnp.float32) + y_sum[1].astype(jnp.float32)
    )

    def finish(h):
        whole[h].wait_recv()
        one[h].wait_recv()
        rows = slice(h * HALF, (h + 1) * HALF)
        part = jnp.zeros((HALF, 128), jnp.float32)
        for k in range(COLS // 128):
            at = slice(k * 128, (k + 1) * 128)
            summed = (
                p_own[2 * OWN + h * HALF:2 * OWN + (h + 1) * HALF, at]
                + rs_one[h, :, at].astype(jnp.float32) + rs_sum[h, :, at].astype(jnp.float32)
            )
            wg_out[rows, at] = summed * ins[rows, at]
            part = part + summed * fac[rows, at]
        parts[rows, :] = part

    parts[OWN:, :] = jnp.zeros((256 - OWN, 128), jnp.float32)
    finish(0)
    finish(1)
    x_snd[...] = jnp.broadcast_to(
        jnp.sum(jnp.transpose(parts[...]), axis=0, keepdims=True) * GRAD_FACTOR, (8, 256)
    )
    sends = [copy(x_snd, x_rcv.at[k], X_SUM + k, crosses[k]) for k in range(3)]
    for send in sends:
        send.start()

    across.wait_recv()
    ig_out[...] = (mine[...] + z_rcv[...].astype(jnp.float32)).astype(jnp.bfloat16)

    for item in list(swap.values()) + list(ig.values()) + own + fwd + aside + far + one + whole + shares + [across]:
        item.wait_send()
    for b in range(4):
        to_peer(b).wait_send()

    for send in sends:
        send.wait_recv()
    total = x_snd[...] + x_rcv[0] + x_rcv[1] + x_rcv[2]
    sg_out[...] = total[0:1, 0:OWN]
    for send in sends:
        send.wait_send()


def store(ig_ref, wg_ref, sg_ref, ig_hbm, wg_hbm, sg_hbm, sems):
    moves = [
        pltpu.make_async_copy(wg_ref, wg_hbm, sems.at[0]),
        pltpu.make_async_copy(ig_ref, ig_hbm, sems.at[1]),
        pltpu.make_async_copy(sg_ref, sg_hbm, sems.at[2]),
    ]
    for move in moves:
        move.start()
    for move in moves:
        move.wait()


def shards(activations, out_grad, weight, step_size):
    bf16, f32 = jnp.bfloat16, jnp.float32
    hbm = pl.BlockSpec(memory_space=pltpu.HBM)
    vmem = pl.BlockSpec(memory_space=pltpu.VMEM)
    input_grad, weight_grad, step_rows = pl.pallas_call(
        kernel,
        out_shape=(
            pltpu.VMEM((SUB, COLS), bf16),
            pltpu.VMEM((OWN, COLS), f32),
            pltpu.VMEM((1, OWN), f32),
        ),
        in_specs=[hbm] * 4,
        out_specs=(vmem, vmem, vmem),
        scratch_shapes=[
            pltpu.VMEM((TOKENS, COLS), bf16),
            pltpu.VMEM((TOKENS, ROWS), bf16),
            pltpu.VMEM((OWN, COLS), f32),
            pltpu.VMEM((1, ROWS), f32),
            pltpu.VMEM((ROWS, 128), f32),
            pltpu.VMEM((ROWS, TOKENS), bf16),
            pltpu.VMEM((2 * OWN, TOKENS), bf16),
            pltpu.VMEM((ROWS, COLS), bf16),
            pltpu.VMEM((OWN, COLS), f32),
            pltpu.VMEM((OWN, COLS), f32),
            pltpu.VMEM((4 * OWN, COLS), f32),
            pltpu.VMEM((4 * OWN, COLS), bf16),
            pltpu.VMEM((4 * OWN, COLS), bf16),
            pltpu.VMEM((4 * OWN, COLS), bf16),
            pltpu.VMEM((2, HALF, COLS), bf16),
            pltpu.VMEM((2, HALF, COLS), bf16),
            pltpu.VMEM((2, HALF, COLS), bf16),
            pltpu.VMEM((2, HALF, COLS), bf16),
            pltpu.VMEM((256, 128), f32),
            pltpu.VMEM((TOKENS, COLS), bf16),
            pltpu.VMEM((2 * SUB, COLS), f32),
            pltpu.VMEM((2, SUB, COLS), bf16),
            pltpu.VMEM((2, SUB, COLS), bf16),
            pltpu.VMEM((2, SUB, COLS), bf16),
            pltpu.VMEM((2, SUB, COLS), bf16),
            pltpu.VMEM((SUB, COLS), f32),
            pltpu.VMEM((SUB, COLS), bf16),
            pltpu.VMEM((SUB, COLS), bf16),
            pltpu.VMEM((8, 256), f32),
            pltpu.VMEM((3, 8, 256), f32),
            pltpu.SemaphoreType.DMA((N_COPIES,)),
            pltpu.SemaphoreType.DMA((N_COPIES,)),
            pltpu.SemaphoreType.DMA((4,)),
        ],
        compiler_params=pltpu.CompilerParams(
            collective_id=0, has_side_effects=True, vmem_limit_bytes=60*1024*1024
        ),
        name="backward",
    )(activations, out_grad, weight[0], step_size)
    outs = pl.pallas_call(
        store,
        out_shape=(
            jax.ShapeDtypeStruct((SUB, COLS), bf16),
            jax.ShapeDtypeStruct((OWN, COLS), f32),
            jax.ShapeDtypeStruct((1, OWN), f32),
        ),
        in_specs=[vmem] * 3,
        out_specs=(hbm,) * 3,
        scratch_shapes=[pltpu.SemaphoreType.DMA((3,))],
        compiler_params=pltpu.CompilerParams(vmem_limit_bytes=4 * 1024 * 1024),
        name="store",
    )(input_grad, weight_grad, step_rows)
    return (outs[0], outs[1][None], outs[2])


def solution(mesh):
    split = Mesh(mesh.devices.reshape(4, 2, 4, 2, 4), ("zh", "core", "y", "zl", "x"))
    in_specs = (P(DP, "x"), P(DP, ROW), P(ROW, DP, "x"), P(ROW, None))
    out_specs = (P(DP + ROW, "x"), P(ROW, DP, "x"), P(ROW, DP))
    return jax.shard_map(
        shards, mesh=split, in_specs=in_specs, out_specs=out_specs, check_vma=False
    )
```

```python
import functools

import jax
import jax.numpy as jnp
from jax import lax
from jax.experimental import pallas as pl
from jax.experimental.pallas import tpu as pltpu
from jax.sharding import Mesh
from jax.sharding import PartitionSpec as P

MESH = pl.DeviceIdType.MESH
D = 4096
DP = ("zh", "core")
ROW = ("y", "zl")
OWN = 224
HALF = 112
COLS = 1024
ROWS = 1792
TOKENS = 1024
SUB = 128
CHUNKS = ((0, 112), (112, 192), (192, 224))
GRAD_FACTOR = 1.0 / (7.0 * D) ** 0.5

S_MAIN, S_P, S_Y, S_SHARE, S_TURN, S_X, N_SEND = range(7)
(
    R_OWN, _, R_FWD, R_ASIDE, R_SWAP, R_P, R_P3, R_FAR, _, R_SUM, _, R_ONE, _, _,
    R_FP, R_FM, R_PP, R_MM, R_Z, R_X, R_TURN, R_SHARE, N_RECV,
) = range(23)


def rows_of(index, size):
    return pl.ds(pl.multiple_of(index * size, size), size)


def kernel(
    act_hbm, og_hbm, w_hbm, s_hbm,
    ig_out, wg_out, sg_out,
    act, og, w, s, scol, ogt, ogt_pair, q, fac, ins,
    p_own, p_snd, p_rcv, c_buf,
    rs_far, rs_one, rs_sum, rs_snd, parts,
    g, gown, y_far, y_own, y_sum, y_snd, mine, z_snd, z_rcv,
    x_snd, x_rcv,
    ss, rs, ls,
):
    zh = lax.axis_index("zh")
    core = lax.axis_index("core")
    y = lax.axis_index("y")
    zl = lax.axis_index("zl")
    x = lax.axis_index("x")
    zf = (zh + 2) % 4
    zs = (zh + 3 + 2 * zl) % 4
    zo = (zh + 1 + 2 * zl) % 4
    chain, back = {"zh": zs}, {"zh": zo}
    beside = {"zh": zs, "zl": 1 - zl}
    other = 1 - core
    peer = {"core": other}
    yf = (y + 2) % 4
    pair = {"zl": 1 - zl}
    crosses = [{"x": (x + k) % 4} for k in (2, 1, 3)]
    hp = 1 - zl
    yp = (y + 1 + 2 * hp) % 4
    ym = (y + 3 + 2 * hp) % 4
    way_p, way_m = {"y": yp}, {"y": ym}

    loads = [
        pltpu.make_async_copy(s_hbm, s, ls.at[0]),
        pltpu.make_async_copy(w_hbm.at[0:HALF], w.at[0:HALF], ls.at[1]),
        pltpu.make_async_copy(w_hbm.at[HALF:OWN], w.at[HALF:OWN], ls.at[2]),
        pltpu.make_async_copy(og_hbm, og, ls.at[3]),
        pltpu.make_async_copy(act_hbm, act, ls.at[4]),
    ]
    barrier = pltpu.get_barrier_semaphore()
    partners = [chain, back, beside, peer, way_p, way_m, pair] + crosses
    for partner in partners:
        pl.semaphore_signal(barrier, inc=1, device_id=partner, device_id_type=MESH)
    for load in loads[:3]:
        load.start()

    def copy(src, dst, sender, receiver, device):
        return pltpu.make_async_remote_copy(
            src_ref=src, dst_ref=dst, send_sem=ss.at[sender], recv_sem=rs.at[receiver],
            device_id=device, device_id_type=MESH,
        )

    def wait_received(receiver, rows):
        copy(q.at[0:rows], q.at[0:rows], S_MAIN, receiver, peer).wait_recv()

    def wait_sent(sender, rows):
        copy(q.at[0:rows], q.at[0:rows], sender, R_SWAP, peer).wait_send()

    def shard(j):
        return q.at[rows_of(j * 2 + core, OWN)]

    def half(j, h):
        return q.at[rows_of((j * 2 + core) * 2 + h, HALF)]

    first_row = (zh * 2 + core) * OWN
    tile = jnp.minimum(first_row // 128, (ROWS - 3 * 128) // 128)
    loads[0].wait()
    scol[...] = jnp.transpose(
        jnp.broadcast_to(s[:, pl.ds(pl.multiple_of(tile * 128, 128), 3 * 128)], (128, 3 * 128))
    )
    scale_at = first_row - tile * 128

    def quantize(h):
        rows = slice(h * HALF, (h + 1) * HALF)
        scale = scol[pl.ds(pl.multiple_of(scale_at + h * HALF, 16), HALF), :]
        for k in range(COLS // 128):
            at = slice(k * 128, (k + 1) * 128)
            levels = jnp.floor(jnp.clip(w[rows, at] / scale, -8.0, 7.0) + 0.5)
            q[rows_of((zh * 2 + core) * 2 + h, HALF), at] = (levels * scale).astype(jnp.bfloat16)

    loads[1].wait()
    quantize(0)
    pl.semaphore_wait(barrier, len(partners))

    own = [copy(half(zh, h), half(zh, h), S_MAIN, R_OWN + h, back) for h in range(2)]
    fwd = [copy(half(zs, h), half(zs, h), S_MAIN, R_FWD, back) for h in range(2)]
    aside = [copy(half(zh, h), half(zf, h), S_MAIN, R_ASIDE, beside) for h in range(2)]

    def swap(j):
        return copy(shard(j), shard(j), S_MAIN, R_SWAP, peer)

    own[0].start()
    aside[0].start()
    loads[3].start()
    loads[4].start()
    loads[2].wait()
    quantize(1)

    loads[3].wait()
    aside[1].start()
    swap(zh).start()
    for k in range(ROWS // 128):
        at = slice(k * 128, (k + 1) * 128)
        ogt[at, :] = jnp.transpose(og[:, at])

    quarter = ogt_pair.at[rows_of(x, HALF)]
    turned = copy(ogt.at[rows_of(zo * 4 + x, HALF)], quarter, S_TURN, R_TURN, pair)
    turned.start()
    own[1].start()

    scale = scol[pl.ds(pl.multiple_of(scale_at, 16), OWN), :]
    for k in range(COLS // 128):
        at = slice(k * 128, (k + 1) * 128)
        ratio = w[:, at] / scale
        clipped = jnp.clip(ratio, -8.0, 7.0)
        levels = jnp.floor(clipped + 0.5)
        inside = (ratio >= -8.0) & (ratio <= 7.0)
        ins[:, at] = jnp.where(inside, 1.0, 0.0)
        fac[:, at] = jnp.where(inside, levels - ratio, clipped)

    loads[4].wait()

    def product(at, c, n):
        return jnp.dot(
            ogt[rows_of(at * 2 + c, OWN), :], act[:, n * 256:(n + 1) * 256],
            preferred_element_type=jnp.float32,
        )

    def to_peer(b, receiver):
        return copy(
            p_snd.at[rows_of(b, OWN)], p_rcv.at[rows_of(b, OWN)], S_P, receiver, peer
        )

    @pl.loop(0, 3)
    def _(b):
        dest = jnp.where(b == 0, zf, jnp.where(b == 1, zs, zh))
        for n in range(4):
            at = slice(n * 256, (n + 1) * 256)
            p_snd[rows_of(b, OWN), at] = product(dest, other, n).astype(jnp.bfloat16)
        for n in range(4):
            at = slice(n * 256, (n + 1) * 256)
            p_own[rows_of(b, OWN), at] = product(dest, core, n)
        to_peer(b, R_P).start()

    def chip_sum(b):
        at = rows_of(b, OWN)
        total = p_own[at, :] + p_rcv[at, :].astype(jnp.float32)
        p_own[at, :] = total
        c_buf[at, :] = total.astype(jnp.bfloat16)

    own[0].wait_recv()
    fwd[0].start()

    wait_received(R_P, 3 * OWN)

    @pl.loop(0, 3)
    def _(b):
        chip_sum(b)

    def c_half(b, h):
        return c_buf.at[(2 * b + h) * HALF:(2 * b + h + 1) * HALF]

    far = [copy(c_half(0, h), rs_far.at[h], S_MAIN, R_FAR + h, chain) for h in range(2)]
    one = [
        copy(c_buf.at[3 * OWN + i:3 * OWN + j], rs_one.at[i:j], S_P, R_ONE + n, beside)
        for n, (i, j) in enumerate(CHUNKS)
    ]
    whole = [copy(rs_snd.at[h], rs_sum.at[h * HALF:(h + 1) * HALF], S_P, R_SUM + h, chain) for h in range(2)]

    for item in far:
        item.start()

    turned.wait_recv()
    shares = [copy(quarter, quarter, S_SHARE, R_SHARE, cross) for cross in crosses]
    for share in shares:
        share.start()
    own[1].wait_recv()
    fwd[1].start()
    swap(zs).start()

    wait_received(R_SHARE, 3 * HALF)
    turned.wait_send()
    ogt[rows_of(zo, 2 * OWN), :] = ogt_pair[...]
    for n in range(4):
        at = slice(n * 256, (n + 1) * 256)
        p_snd[3 * OWN:, at] = product(zo, other, n).astype(jnp.bfloat16)
    for n in range(4):
        at = slice(n * 256, (n + 1) * 256)
        p_own[3 * OWN:, at] = product(zo, core, n)
    last = to_peer(3, R_P3)
    last.start()
    for k in range(ROWS // 128):
        at = slice(k * 128, (k + 1) * 128)
        og[:, at] = jnp.transpose(ogt[at, :])
    last.wait_recv()
    chip_sum(3)

    one[0].start()
    wait_received(R_ASIDE, OWN)
    swap(zo).start()
    wait_received(R_FWD, OWN)
    swap(zf).start()
    wait_received(R_SWAP, 4 * OWN)

    def g_half(j, h):
        return g.at[rows_of(j * 2 + h, SUB)]

    far_p = copy(g_half(yf, hp), y_far.at[0], S_Y, R_FP, way_p)
    far_m = copy(g_half(yf, zl), y_far.at[1], S_Y, R_FM, way_m)
    own_p = copy(g_half(ym, hp), y_own.at[0], S_Y, R_PP, way_m)
    own_m = copy(g_half(yp, zl), y_own.at[1], S_Y, R_MM, way_p)
    sum_p = copy(y_snd.at[0], y_sum.at[0], S_Y, R_PP, way_p)
    sum_m = copy(y_snd.at[1], y_sum.at[1], S_Y, R_MM, way_m)

    def block(t, n):
        return jnp.dot(
            og[rows_of(t, 2 * SUB), :], q[:, n * 256:(n + 1) * 256],
            preferred_element_type=jnp.float32,
        )

    @pl.loop(0, 3)
    def _(k):
        t = jnp.where(k == 0, yf, jnp.where(k == 1, ym, yp))
        for n in range(4):
            g[rows_of(t, 2 * SUB), n * 256:(n + 1) * 256] = block(t, n).astype(jnp.bfloat16)

        @pl.when(k == 0)
        def _():
            far_p.start()
            far_m.start()

        @pl.when(k == 1)
        def _():
            own_p.start()

    for n in range(4):
        gown[:, n * 256:(n + 1) * 256] = block(y, n)

    def middle(h):
        far[h].wait_recv()
        rs_snd[h] = (
            p_own[OWN + h * HALF:OWN + (h + 1) * HALF, :] + rs_far[h].astype(jnp.float32)
        ).astype(jnp.bfloat16)
        whole[h].start()

    middle(0)
    far_p.wait_recv()
    y_snd[0] = (
        g[rows_of(yp * 2 + hp, SUB), :].astype(jnp.float32) + y_far[0].astype(jnp.float32)
    ).astype(jnp.bfloat16)
    sum_p.start()
    own_m.start()

    far_m.wait_recv()
    y_snd[1] = (
        g[rows_of(ym * 2 + zl, SUB), :].astype(jnp.float32) + y_far[1].astype(jnp.float32)
    ).astype(jnp.bfloat16)
    sum_m.start()
    middle(1)
    one[1].start()
    one[2].start()

    wait_received(R_PP, 2 * SUB)
    z_snd[...] = (
        gown[rows_of(hp, SUB), :] + y_own[0].astype(jnp.float32) + y_sum[0].astype(jnp.float32)
    ).astype(jnp.bfloat16)
    across = copy(z_snd, z_rcv, S_Y, R_Z, pair)
    across.start()
    wait_received(R_MM, 2 * SUB)
    mine[...] = (
        gown[rows_of(zl, SUB), :] + y_own[1].astype(jnp.float32) + y_sum[1].astype(jnp.float32)
    )

    def finish(n):
        i, j = CHUNKS[n]
        one[n].wait_recv()
        part = jnp.zeros((j - i, 128), jnp.float32)
        for k in range(COLS // 128):
            at = slice(k * 128, (k + 1) * 128)
            summed = (
                p_own[2 * OWN + i:2 * OWN + j, at]
                + rs_one[i:j, at].astype(jnp.float32) + rs_sum[i:j, at].astype(jnp.float32)
            )
            wg_out[i:j, at] = summed * ins[i:j, at]
            part = part + summed * fac[i:j, at]
        parts[i:j, :] = part

    def row_sums(h):
        at = slice(h * 128, (h + 1) * 128)
        x_snd[:, at] = jnp.broadcast_to(
            jnp.sum(jnp.transpose(parts[at, :]), axis=0, keepdims=True) * GRAD_FACTOR, (8, 128)
        )

    parts[OWN:, :] = jnp.zeros((256 - OWN, 128), jnp.float32)
    whole[0].wait_recv()
    finish(0)
    whole[1].wait_recv()
    finish(1)
    row_sums(0)
    finish(2)
    row_sums(1)
    sends = [copy(x_snd, x_rcv.at[k], S_X, R_X, crosses[k]) for k in range(3)]
    for send in sends:
        send.start()

    across.wait_recv()
    ig_out[...] = (mine[...] + z_rcv[...].astype(jnp.float32)).astype(jnp.bfloat16)

    wait_sent(S_MAIN, ROWS)
    wait_sent(S_P, 6 * OWN)
    wait_sent(S_Y, 7 * SUB)
    wait_sent(S_SHARE, 3 * HALF)

    both = copy(x_rcv, x_rcv, S_X, R_X, peer)
    both.wait_recv()
    total = x_snd[...] + x_rcv[0] + x_rcv[1] + x_rcv[2]
    sg_out[...] = total[0:1, 0:OWN]
    both.wait_send()


def store(ig_ref, wg_ref, sg_ref, ig_hbm, wg_hbm, sg_hbm, sems):
    moves = [
        pltpu.make_async_copy(wg_ref.at[i:i + 56], wg_hbm.at[i:i + 56], sems.at[i // 56])
        for i in range(0, OWN, 56)
    ] + [
        pltpu.make_async_copy(ig_ref, ig_hbm, sems.at[4]),
        pltpu.make_async_copy(sg_ref, sg_hbm, sems.at[5]),
    ]
    for move in moves:
        move.start()
    for move in moves:
        move.wait()


def shards(activations, out_grad, weight, step_size):
    bf16, f32 = jnp.bfloat16, jnp.float32
    hbm = pl.BlockSpec(memory_space=pltpu.HBM)
    vmem = pl.BlockSpec(memory_space=pltpu.VMEM)
    input_grad, weight_grad, step_rows = pl.pallas_call(
        kernel,
        out_shape=(
            pltpu.VMEM((SUB, COLS), bf16),
            pltpu.VMEM((OWN, COLS), f32),
            pltpu.VMEM((1, OWN), f32),
        ),
        in_specs=[hbm] * 4,
        out_specs=(vmem, vmem, vmem),
        scratch_shapes=[
            pltpu.VMEM((TOKENS, COLS), bf16),
            pltpu.VMEM((TOKENS, ROWS), bf16),
            pltpu.VMEM((OWN, COLS), f32),
            pltpu.VMEM((1, ROWS), f32),
            pltpu.VMEM((3 * 128, 128), f32),
            pltpu.VMEM((ROWS, TOKENS), bf16),
            pltpu.VMEM((2 * OWN, TOKENS), bf16),
            pltpu.VMEM((ROWS, COLS), bf16),
            pltpu.VMEM((OWN, COLS), f32),
            pltpu.VMEM((OWN, COLS), f32),
            pltpu.VMEM((4 * OWN, COLS), f32),
            pltpu.VMEM((4 * OWN, COLS), bf16),
            pltpu.VMEM((4 * OWN, COLS), bf16),
            pltpu.VMEM((4 * OWN, COLS), bf16),
            pltpu.VMEM((2, HALF, COLS), bf16),
            pltpu.VMEM((OWN, COLS), bf16),
            pltpu.VMEM((OWN, COLS), bf16),
            pltpu.VMEM((2, HALF, COLS), bf16),
            pltpu.VMEM((256, 128), f32),
            pltpu.VMEM((TOKENS, COLS), bf16),
            pltpu.VMEM((2 * SUB, COLS), f32),
            pltpu.VMEM((2, SUB, COLS), bf16),
            pltpu.VMEM((2, SUB, COLS), bf16),
            pltpu.VMEM((2, SUB, COLS), bf16),
            pltpu.VMEM((2, SUB, COLS), bf16),
            pltpu.VMEM((SUB, COLS), f32),
            pltpu.VMEM((SUB, COLS), bf16),
            pltpu.VMEM((SUB, COLS), bf16),
            pltpu.VMEM((8, 256), f32),
            pltpu.VMEM((3, 8, 256), f32),
            pltpu.SemaphoreType.DMA((N_SEND,)),
            pltpu.SemaphoreType.DMA((N_RECV,)),
            pltpu.SemaphoreType.DMA((5,)),
        ],
        compiler_params=pltpu.CompilerParams(
            collective_id=0, has_side_effects=True, vmem_limit_bytes=60*1024*1024
        ),
        name="backward",
    )(activations, out_grad, weight[0], step_size)
    outs = pl.pallas_call(
        store,
        out_shape=(
            jax.ShapeDtypeStruct((SUB, COLS), bf16),
            jax.ShapeDtypeStruct((OWN, COLS), f32),
            jax.ShapeDtypeStruct((1, OWN), f32),
        ),
        in_specs=[vmem] * 3,
        out_specs=(hbm,) * 3,
        scratch_shapes=[pltpu.SemaphoreType.DMA((6,))],
        compiler_params=pltpu.CompilerParams(vmem_limit_bytes=4 * 1024 * 1024),
        name="store",
    )(input_grad, weight_grad, step_rows)
    return (outs[0], outs[1][None], outs[2])


def solution(mesh):
    split = Mesh(mesh.devices.reshape(4, 2, 4, 2, 4), ("zh", "core", "y", "zl", "x"))
    in_specs = (P(DP, "x"), P(DP, ROW), P(ROW, DP, "x"), P(ROW, None))
    out_specs = (P(DP + ROW, "x"), P(ROW, DP, "x"), P(ROW, DP))
    return jax.shard_map(
        shards, mesh=split, in_specs=in_specs, out_specs=out_specs, check_vma=False
    )
```

```python
import functools

import jax
import jax.numpy as jnp
from jax import lax
from jax.experimental import pallas as pl
from jax.experimental.pallas import tpu as pltpu
from jax.sharding import Mesh
from jax.sharding import PartitionSpec as P

MESH = pl.DeviceIdType.MESH
D = 4096
DP = ("zh", "core")
ROW = ("y", "zl")
OWN = 224
HALF = 112
COLS = 1024
ROWS = 1792
TOKENS = 1024
SUB = 128
CHUNKS = ((0, 112), (112, 192), (192, 224))
GRAD_FACTOR = 1.0 / (7.0 * D) ** 0.5

S_MAIN, S_P, S_Y, S_SHARE, S_TURN, S_X, N_SEND = range(7)
(
    R_OWN, _, R_FWD, R_ASIDE, R_SWAP, R_P, R_P3, R_FAR, _, R_SUM, _, R_ONE, _, _,
    R_FP, R_FM, R_PP, R_MM, R_Z, R_X, R_TURN, R_SHARE, N_RECV,
) = range(23)


def rows_of(index, size):
    return pl.ds(pl.multiple_of(index * size, size), size)


def kernel(
    act_hbm, og_hbm, w_hbm, s_hbm,
    ig_out, wg_out, sg_out,
    act, og, w, s, scol, ogt, ogt_pair, q, fac, ins,
    p_own, p_snd, p_rcv, c_buf,
    rs_far, rs_one, rs_sum, rs_snd, parts,
    g, gown, y_far, y_own, y_sum, y_snd, mine, z_snd, z_rcv,
    x_snd, x_rcv,
    ss, rs, ls, told,
):
    zh = lax.axis_index("zh")
    core = lax.axis_index("core")
    y = lax.axis_index("y")
    zl = lax.axis_index("zl")
    x = lax.axis_index("x")
    zf = (zh + 2) % 4
    zs = (zh + 3 + 2 * zl) % 4
    zo = (zh + 1 + 2 * zl) % 4
    chain, back = {"zh": zs}, {"zh": zo}
    beside = {"zh": zs, "zl": 1 - zl}
    other = 1 - core
    peer = {"core": other}
    yf = (y + 2) % 4
    pair = {"zl": 1 - zl}
    crosses = [{"x": (x + k) % 4} for k in (2, 1, 3)]
    hp = 1 - zl
    yp = (y + 1 + 2 * hp) % 4
    ym = (y + 3 + 2 * hp) % 4
    way_p, way_m = {"y": yp}, {"y": ym}

    loads = [
        pltpu.make_async_copy(s_hbm, s, ls.at[0]),
        pltpu.make_async_copy(w_hbm.at[0:HALF], w.at[0:HALF], ls.at[1]),
        pltpu.make_async_copy(w_hbm.at[HALF:OWN], w.at[HALF:OWN], ls.at[2]),
        pltpu.make_async_copy(og_hbm, og, ls.at[3]),
        pltpu.make_async_copy(act_hbm, act, ls.at[4]),
    ]
    barrier = pltpu.get_barrier_semaphore()
    along_z = [chain, back, beside, pair]
    across_z = [way_p, way_m] + crosses
    for partner in along_z:
        pl.semaphore_signal(barrier, inc=1, device_id={**partner, "core": 1}, device_id_type=MESH)

    @pl.when(core == 0)
    def _():
        pl.semaphore_signal(barrier, inc=1, device_id=peer, device_id_type=MESH)

    for partner in across_z:
        pl.semaphore_signal(barrier, inc=1, device_id={**partner, "core": 0}, device_id_type=MESH)

    def meet(listener, signals):
        @pl.when(core == listener)
        def _():
            pl.semaphore_wait(barrier, signals)
            pl.semaphore_signal(told, inc=1, device_id=peer, device_id_type=MESH)

        @pl.when(core != listener)
        def _():
            pl.semaphore_wait(told, 1)

    for load in loads[:3]:
        load.start()

    def copy(src, dst, sender, receiver, device):
        return pltpu.make_async_remote_copy(
            src_ref=src, dst_ref=dst, send_sem=ss.at[sender], recv_sem=rs.at[receiver],
            device_id=device, device_id_type=MESH,
        )

    def wait_received(receiver, rows):
        copy(q.at[0:rows], q.at[0:rows], S_MAIN, receiver, peer).wait_recv()

    def wait_sent(sender, rows):
        copy(q.at[0:rows], q.at[0:rows], sender, R_SWAP, peer).wait_send()

    def shard(j):
        return q.at[rows_of(j * 2 + core, OWN)]

    def half(j, h):
        return q.at[rows_of((j * 2 + core) * 2 + h, HALF)]

    first_row = (zh * 2 + core) * OWN
    tile = jnp.minimum(first_row // 128, (ROWS - 3 * 128) // 128)
    loads[0].wait()
    scol[...] = jnp.transpose(
        jnp.broadcast_to(s[:, pl.ds(pl.multiple_of(tile * 128, 128), 3 * 128)], (128, 3 * 128))
    )
    scale_at = first_row - tile * 128

    def quantize(h):
        rows = slice(h * HALF, (h + 1) * HALF)
        scale = scol[pl.ds(pl.multiple_of(scale_at + h * HALF, 16), HALF), :]
        for k in range(COLS // 128):
            at = slice(k * 128, (k + 1) * 128)
            levels = jnp.floor(jnp.clip(w[rows, at] / scale, -8.0, 7.0) + 0.5)
            q[rows_of((zh * 2 + core) * 2 + h, HALF), at] = (levels * scale).astype(jnp.bfloat16)

    loads[1].wait()
    quantize(0)
    meet(1, 2 * len(along_z) + 1)

    own = [copy(half(zh, h), half(zh, h), S_MAIN, R_OWN + h, back) for h in range(2)]
    fwd = [copy(half(zs, h), half(zs, h), S_MAIN, R_FWD, back) for h in range(2)]
    aside = [copy(half(zh, h), half(zf, h), S_MAIN, R_ASIDE, beside) for h in range(2)]

    def swap(j):
        return copy(shard(j), shard(j), S_MAIN, R_SWAP, peer)

    own[0].start()
    aside[0].start()
    loads[3].start()
    loads[4].start()
    loads[2].wait()
    quantize(1)

    loads[3].wait()
    aside[1].start()
    swap(zh).start()
    for k in range(ROWS // 128):
        at = slice(k * 128, (k + 1) * 128)
        ogt[at, :] = jnp.transpose(og[:, at])

    quarter = ogt_pair.at[rows_of(x, HALF)]
    turned = copy(ogt.at[rows_of(zo * 4 + x, HALF)], quarter, S_TURN, R_TURN, pair)
    turned.start()
    own[1].start()

    scale = scol[pl.ds(pl.multiple_of(scale_at, 16), OWN), :]
    for k in range(COLS // 128):
        at = slice(k * 128, (k + 1) * 128)
        ratio = w[:, at] / scale
        clipped = jnp.clip(ratio, -8.0, 7.0)
        levels = jnp.floor(clipped + 0.5)
        inside = (ratio >= -8.0) & (ratio <= 7.0)
        ins[:, at] = jnp.where(inside, 1.0, 0.0)
        fac[:, at] = jnp.where(inside, levels - ratio, clipped)

    loads[4].wait()

    def product(at, c, n):
        return jnp.dot(
            ogt[rows_of(at * 2 + c, OWN), :], act[:, n * 256:(n + 1) * 256],
            preferred_element_type=jnp.float32,
        )

    def to_peer(b, receiver):
        return copy(
            p_snd.at[rows_of(b, OWN)], p_rcv.at[rows_of(b, OWN)], S_P, receiver, peer
        )

    @pl.loop(0, 3)
    def _(b):
        dest = jnp.where(b == 0, zf, jnp.where(b == 1, zs, zh))
        for n in range(4):
            at = slice(n * 256, (n + 1) * 256)
            p_snd[rows_of(b, OWN), at] = product(dest, other, n).astype(jnp.bfloat16)
        for n in range(4):
            at = slice(n * 256, (n + 1) * 256)
            p_own[rows_of(b, OWN), at] = product(dest, core, n)
        to_peer(b, R_P).start()

    def chip_sum(b):
        at = rows_of(b, OWN)
        total = p_own[at, :] + p_rcv[at, :].astype(jnp.float32)
        p_own[at, :] = total
        c_buf[at, :] = total.astype(jnp.bfloat16)

    own[0].wait_recv()
    fwd[0].start()

    wait_received(R_P, 3 * OWN)

    @pl.loop(0, 3)
    def _(b):
        chip_sum(b)

    def c_half(b, h):
        return c_buf.at[(2 * b + h) * HALF:(2 * b + h + 1) * HALF]

    far = [copy(c_half(0, h), rs_far.at[h], S_MAIN, R_FAR + h, chain) for h in range(2)]
    one = [
        copy(c_buf.at[3 * OWN + i:3 * OWN + j], rs_one.at[i:j], S_P, R_ONE + n, beside)
        for n, (i, j) in enumerate(CHUNKS)
    ]
    whole = [copy(rs_snd.at[h], rs_sum.at[h * HALF:(h + 1) * HALF], S_P, R_SUM + h, chain) for h in range(2)]

    for item in far:
        item.start()

    turned.wait_recv()
    shares = [copy(quarter, quarter, S_SHARE, R_SHARE, cross) for cross in crosses]
    meet(0, 2 * len(across_z))
    for share in shares:
        share.start()
    own[1].wait_recv()
    fwd[1].start()
    swap(zs).start()

    wait_received(R_SHARE, 3 * HALF)
    turned.wait_send()
    ogt[rows_of(zo, 2 * OWN), :] = ogt_pair[...]
    for n in range(4):
        at = slice(n * 256, (n + 1) * 256)
        p_snd[3 * OWN:, at] = product(zo, other, n).astype(jnp.bfloat16)
    for n in range(4):
        at = slice(n * 256, (n + 1) * 256)
        p_own[3 * OWN:, at] = product(zo, core, n)
    last = to_peer(3, R_P3)
    last.start()
    for k in range(ROWS // 128):
        at = slice(k * 128, (k + 1) * 128)
        og[:, at] = jnp.transpose(ogt[at, :])
    last.wait_recv()
    chip_sum(3)

    one[0].start()
    wait_received(R_ASIDE, OWN)
    swap(zo).start()
    wait_received(R_FWD, OWN)
    swap(zf).start()
    wait_received(R_SWAP, 4 * OWN)

    def g_half(j, h):
        return g.at[rows_of(j * 2 + h, SUB)]

    far_p = copy(g_half(yf, hp), y_far.at[0], S_Y, R_FP, way_p)
    far_m = copy(g_half(yf, zl), y_far.at[1], S_Y, R_FM, way_m)
    own_p = copy(g_half(ym, hp), y_own.at[0], S_Y, R_PP, way_m)
    own_m = copy(g_half(yp, zl), y_own.at[1], S_Y, R_MM, way_p)
    sum_p = copy(y_snd.at[0], y_sum.at[0], S_Y, R_PP, way_p)
    sum_m = copy(y_snd.at[1], y_sum.at[1], S_Y, R_MM, way_m)

    def block(t, n):
        return jnp.dot(
            og[rows_of(t, 2 * SUB), :], q[:, n * 256:(n + 1) * 256],
            preferred_element_type=jnp.float32,
        )

    @pl.loop(0, 3)
    def _(k):
        t = jnp.where(k == 0, yf, jnp.where(k == 1, ym, yp))
        for n in range(4):
            g[rows_of(t, 2 * SUB), n * 256:(n + 1) * 256] = block(t, n).astype(jnp.bfloat16)

        @pl.when(k == 0)
        def _():
            far_p.start()
            far_m.start()

        @pl.when(k == 1)
        def _():
            own_p.start()

    for n in range(4):
        gown[:, n * 256:(n + 1) * 256] = block(y, n)

    def middle(h):
        far[h].wait_recv()
        rs_snd[h] = (
            p_own[OWN + h * HALF:OWN + (h + 1) * HALF, :] + rs_far[h].astype(jnp.float32)
        ).astype(jnp.bfloat16)
        whole[h].start()

    middle(0)
    far_p.wait_recv()
    y_snd[0] = (
        g[rows_of(yp * 2 + hp, SUB), :].astype(jnp.float32) + y_far[0].astype(jnp.float32)
    ).astype(jnp.bfloat16)
    sum_p.start()
    own_m.start()

    far_m.wait_recv()
    y_snd[1] = (
        g[rows_of(ym * 2 + zl, SUB), :].astype(jnp.float32) + y_far[1].astype(jnp.float32)
    ).astype(jnp.bfloat16)
    sum_m.start()
    middle(1)
    one[1].start()
    one[2].start()

    wait_received(R_PP, 2 * SUB)
    z_snd[...] = (
        gown[rows_of(hp, SUB), :] + y_own[0].astype(jnp.float32) + y_sum[0].astype(jnp.float32)
    ).astype(jnp.bfloat16)
    across = copy(z_snd, z_rcv, S_Y, R_Z, pair)
    across.start()
    wait_received(R_MM, 2 * SUB)
    mine[...] = (
        gown[rows_of(zl, SUB), :] + y_own[1].astype(jnp.float32) + y_sum[1].astype(jnp.float32)
    )

    def finish(n):
        i, j = CHUNKS[n]
        one[n].wait_recv()
        part = jnp.zeros((j - i, 128), jnp.float32)
        for k in range(COLS // 128):
            at = slice(k * 128, (k + 1) * 128)
            summed = (
                p_own[2 * OWN + i:2 * OWN + j, at]
                + rs_one[i:j, at].astype(jnp.float32) + rs_sum[i:j, at].astype(jnp.float32)
            )
            wg_out[i:j, at] = summed * ins[i:j, at]
            part = part + summed * fac[i:j, at]
        parts[i:j, :] = part

    def row_sums(h):
        at = slice(h * 128, (h + 1) * 128)
        x_snd[:, at] = jnp.broadcast_to(
            jnp.sum(jnp.transpose(parts[at, :]), axis=0, keepdims=True) * GRAD_FACTOR, (8, 128)
        )

    parts[OWN:, :] = jnp.zeros((256 - OWN, 128), jnp.float32)
    whole[0].wait_recv()
    finish(0)
    whole[1].wait_recv()
    finish(1)
    row_sums(0)
    finish(2)
    row_sums(1)
    sends = [copy(x_snd, x_rcv.at[k], S_X, R_X, crosses[k]) for k in range(3)]
    for send in sends:
        send.start()

    across.wait_recv()
    ig_out[...] = (mine[...] + z_rcv[...].astype(jnp.float32)).astype(jnp.bfloat16)

    wait_sent(S_MAIN, ROWS)
    wait_sent(S_P, 6 * OWN)
    wait_sent(S_Y, 7 * SUB)
    wait_sent(S_SHARE, 3 * HALF)

    both = copy(x_rcv, x_rcv, S_X, R_X, peer)
    both.wait_recv()
    total = x_snd[...] + x_rcv[0] + x_rcv[1] + x_rcv[2]
    sg_out[...] = total[0:1, 0:OWN]
    both.wait_send()


def store(ig_ref, wg_ref, sg_ref, ig_hbm, wg_hbm, sg_hbm, sems):
    moves = [
        pltpu.make_async_copy(wg_ref.at[i:i + 56], wg_hbm.at[i:i + 56], sems.at[i // 56])
        for i in range(0, OWN, 56)
    ] + [
        pltpu.make_async_copy(ig_ref, ig_hbm, sems.at[4]),
        pltpu.make_async_copy(sg_ref, sg_hbm, sems.at[5]),
    ]
    for move in moves:
        move.start()
    for move in moves:
        move.wait()


def shards(activations, out_grad, weight, step_size):
    bf16, f32 = jnp.bfloat16, jnp.float32
    hbm = pl.BlockSpec(memory_space=pltpu.HBM)
    vmem = pl.BlockSpec(memory_space=pltpu.VMEM)
    input_grad, weight_grad, step_rows = pl.pallas_call(
        kernel,
        out_shape=(
            pltpu.VMEM((SUB, COLS), bf16),
            pltpu.VMEM((OWN, COLS), f32),
            pltpu.VMEM((1, OWN), f32),
        ),
        in_specs=[hbm] * 4,
        out_specs=(vmem, vmem, vmem),
        scratch_shapes=[
            pltpu.VMEM((TOKENS, COLS), bf16),
            pltpu.VMEM((TOKENS, ROWS), bf16),
            pltpu.VMEM((OWN, COLS), f32),
            pltpu.VMEM((1, ROWS), f32),
            pltpu.VMEM((3 * 128, 128), f32),
            pltpu.VMEM((ROWS, TOKENS), bf16),
            pltpu.VMEM((2 * OWN, TOKENS), bf16),
            pltpu.VMEM((ROWS, COLS), bf16),
            pltpu.VMEM((OWN, COLS), f32),
            pltpu.VMEM((OWN, COLS), f32),
            pltpu.VMEM((4 * OWN, COLS), f32),
            pltpu.VMEM((4 * OWN, COLS), bf16),
            pltpu.VMEM((4 * OWN, COLS), bf16),
            pltpu.VMEM((4 * OWN, COLS), bf16),
            pltpu.VMEM((2, HALF, COLS), bf16),
            pltpu.VMEM((OWN, COLS), bf16),
            pltpu.VMEM((OWN, COLS), bf16),
            pltpu.VMEM((2, HALF, COLS), bf16),
            pltpu.VMEM((256, 128), f32),
            pltpu.VMEM((TOKENS, COLS), bf16),
            pltpu.VMEM((2 * SUB, COLS), f32),
            pltpu.VMEM((2, SUB, COLS), bf16),
            pltpu.VMEM((2, SUB, COLS), bf16),
            pltpu.VMEM((2, SUB, COLS), bf16),
            pltpu.VMEM((2, SUB, COLS), bf16),
            pltpu.VMEM((SUB, COLS), f32),
            pltpu.VMEM((SUB, COLS), bf16),
            pltpu.VMEM((SUB, COLS), bf16),
            pltpu.VMEM((8, 256), f32),
            pltpu.VMEM((3, 8, 256), f32),
            pltpu.SemaphoreType.DMA((N_SEND,)),
            pltpu.SemaphoreType.DMA((N_RECV,)),
            pltpu.SemaphoreType.DMA((5,)),
            pltpu.SemaphoreType.REGULAR,
        ],
        compiler_params=pltpu.CompilerParams(
            collective_id=0, has_side_effects=True, vmem_limit_bytes=60*1024*1024
        ),
        name="backward",
    )(activations, out_grad, weight[0], step_size)
    outs = pl.pallas_call(
        store,
        out_shape=(
            jax.ShapeDtypeStruct((SUB, COLS), bf16),
            jax.ShapeDtypeStruct((OWN, COLS), f32),
            jax.ShapeDtypeStruct((1, OWN), f32),
        ),
        in_specs=[vmem] * 3,
        out_specs=(hbm,) * 3,
        scratch_shapes=[pltpu.SemaphoreType.DMA((6,))],
        compiler_params=pltpu.CompilerParams(vmem_limit_bytes=4 * 1024 * 1024),
        name="store",
    )(input_grad, weight_grad, step_rows)
    return (outs[0], outs[1][None], outs[2])


def solution(mesh):
    split = Mesh(mesh.devices.reshape(4, 2, 4, 2, 4), ("zh", "core", "y", "zl", "x"))
    in_specs = (P(DP, "x"), P(DP, ROW), P(ROW, DP, "x"), P(ROW, None))
    out_specs = (P(DP + ROW, "x"), P(ROW, DP, "x"), P(ROW, DP))
    return jax.shard_map(
        shards, mesh=split, in_specs=in_specs, out_specs=out_specs, check_vma=False
    )
```

```python
import functools

import jax
import jax.numpy as jnp
from jax import lax
from jax.experimental import pallas as pl
from jax.experimental.pallas import tpu as pltpu
from jax.sharding import Mesh
from jax.sharding import PartitionSpec as P

MESH = pl.DeviceIdType.MESH
D = 4096
DP = ("zh", "core")
ROW = ("y", "zl")
OWN = 224
HALF = 112
COLS = 1024
ROWS = 1792
TOKENS = 1024
SUB = 128
CHUNKS = ((0, 112), (112, 192), (192, 224))
GRAD_FACTOR = 1.0 / (7.0 * D) ** 0.5

S_MAIN, S_P, S_Y, S_SHARE, S_TURN, S_X, N_SEND = range(7)
(
    R_OWN, _, R_FWD, R_ASIDE, R_SWAP, R_P, R_P3, R_FAR, _, R_SUM, _, R_ONE, _, _,
    R_FP, R_FM, R_PP, R_MM, R_Z, R_X, R_TURN, R_SHARE, N_RECV,
) = range(23)


def rows_of(index, size):
    return pl.ds(pl.multiple_of(index * size, size), size)


def kernel(
    act_hbm, og_hbm, w_hbm, s_hbm,
    ig_out, wg_out, sg_out,
    act, og, w, s, scol, ogt, ogt_pair, q, fac, ins,
    p_own, p_snd, p_rcv, c_buf,
    rs_far, rs_one, rs_sum, rs_snd, parts,
    g, gown, y_far, y_own, y_sum, y_snd, mine, z_snd, z_rcv,
    x_snd, x_rcv,
    ss, rs, ls, told,
):
    zh = lax.axis_index("zh")
    core = lax.axis_index("core")
    y = lax.axis_index("y")
    zl = lax.axis_index("zl")
    x = lax.axis_index("x")
    zf = (zh + 2) % 4
    zs = (zh + 3 + 2 * zl) % 4
    zo = (zh + 1 + 2 * zl) % 4
    chain, back = {"zh": zs}, {"zh": zo}
    beside = {"zh": zs, "zl": 1 - zl}
    other = 1 - core
    peer = {"core": other}
    yf = (y + 2) % 4
    pair = {"zl": 1 - zl}
    crosses = [{"x": (x + k) % 4} for k in (2, 1, 3)]
    hp = 1 - zl
    yp = (y + 1 + 2 * hp) % 4
    ym = (y + 3 + 2 * hp) % 4
    way_p, way_m = {"y": yp}, {"y": ym}

    loads = [
        pltpu.make_async_copy(s_hbm, s, ls.at[0]),
        pltpu.make_async_copy(w_hbm.at[0:HALF], w.at[0:HALF], ls.at[1]),
        pltpu.make_async_copy(w_hbm.at[HALF:OWN], w.at[HALF:OWN], ls.at[2]),
        pltpu.make_async_copy(og_hbm, og, ls.at[3]),
        pltpu.make_async_copy(act_hbm, act, ls.at[4]),
    ]
    barrier = pltpu.get_barrier_semaphore()
    along_z = [chain, back, beside, pair, peer]
    across_z = [way_p, way_m] + crosses
    for partner in along_z:
        pl.semaphore_signal(barrier, inc=1, device_id=partner, device_id_type=MESH)
    for partner in across_z:
        pl.semaphore_signal(barrier, inc=1, device_id={**partner, "core": 0}, device_id_type=MESH)

    for load in loads[:3]:
        load.start()

    def copy(src, dst, sender, receiver, device):
        return pltpu.make_async_remote_copy(
            src_ref=src, dst_ref=dst, send_sem=ss.at[sender], recv_sem=rs.at[receiver],
            device_id=device, device_id_type=MESH,
        )

    def wait_received(receiver, rows):
        copy(q.at[0:rows], q.at[0:rows], S_MAIN, receiver, peer).wait_recv()

    def wait_sent(sender, rows):
        copy(q.at[0:rows], q.at[0:rows], sender, R_SWAP, peer).wait_send()

    def shard(j):
        return q.at[rows_of(j * 2 + core, OWN)]

    def half(j, h):
        return q.at[rows_of((j * 2 + core) * 2 + h, HALF)]

    first_row = (zh * 2 + core) * OWN
    tile = jnp.minimum(first_row // 128, (ROWS - 3 * 128) // 128)
    loads[0].wait()
    scol[...] = jnp.transpose(
        jnp.broadcast_to(s[:, pl.ds(pl.multiple_of(tile * 128, 128), 3 * 128)], (128, 3 * 128))
    )
    scale_at = first_row - tile * 128

    def quantize(h):
        rows = slice(h * HALF, (h + 1) * HALF)
        scale = scol[pl.ds(pl.multiple_of(scale_at + h * HALF, 16), HALF), :]
        for k in range(COLS // 128):
            at = slice(k * 128, (k + 1) * 128)
            levels = jnp.floor(jnp.clip(w[rows, at] / scale, -8.0, 7.0) + 0.5)
            q[rows_of((zh * 2 + core) * 2 + h, HALF), at] = (levels * scale).astype(jnp.bfloat16)

    loads[1].wait()
    quantize(0)

    @pl.when(core == 1)
    def _():
        pl.semaphore_wait(barrier, len(along_z))

    @pl.when(core == 0)
    def _():
        pl.semaphore_wait(barrier, len(along_z) + 2 * len(across_z))
        pl.semaphore_signal(told, inc=1, device_id=peer, device_id_type=MESH)


    own = [copy(half(zh, h), half(zh, h), S_MAIN, R_OWN + h, back) for h in range(2)]
    fwd = [copy(half(zs, h), half(zs, h), S_MAIN, R_FWD, back) for h in range(2)]
    aside = [copy(half(zh, h), half(zf, h), S_MAIN, R_ASIDE, beside) for h in range(2)]

    def swap(j):
        return copy(shard(j), shard(j), S_MAIN, R_SWAP, peer)

    own[0].start()
    aside[0].start()
    loads[3].start()
    loads[4].start()
    loads[2].wait()
    quantize(1)

    loads[3].wait()
    aside[1].start()
    swap(zh).start()
    for k in range(ROWS // 128):
        at = slice(k * 128, (k + 1) * 128)
        ogt[at, :] = jnp.transpose(og[:, at])

    quarter = ogt_pair.at[rows_of(x, HALF)]
    turned = copy(ogt.at[rows_of(zo * 4 + x, HALF)], quarter, S_TURN, R_TURN, pair)
    turned.start()
    own[1].start()

    scale = scol[pl.ds(pl.multiple_of(scale_at, 16), OWN), :]
    for k in range(COLS // 128):
        at = slice(k * 128, (k + 1) * 128)
        ratio = w[:, at] / scale
        clipped = jnp.clip(ratio, -8.0, 7.0)
        levels = jnp.floor(clipped + 0.5)
        inside = (ratio >= -8.0) & (ratio <= 7.0)
        ins[:, at] = jnp.where(inside, 1.0, 0.0)
        fac[:, at] = jnp.where(inside, levels - ratio, clipped)

    loads[4].wait()

    def product(at, c, n):
        return jnp.dot(
            ogt[rows_of(at * 2 + c, OWN), :], act[:, n * 256:(n + 1) * 256],
            preferred_element_type=jnp.float32,
        )

    def to_peer(b, receiver):
        return copy(
            p_snd.at[rows_of(b, OWN)], p_rcv.at[rows_of(b, OWN)], S_P, receiver, peer
        )

    @pl.loop(0, 3)
    def _(b):
        dest = jnp.where(b == 0, zf, jnp.where(b == 1, zs, zh))
        for n in range(4):
            at = slice(n * 256, (n + 1) * 256)
            p_snd[rows_of(b, OWN), at] = product(dest, other, n).astype(jnp.bfloat16)
        for n in range(4):
            at = slice(n * 256, (n + 1) * 256)
            p_own[rows_of(b, OWN), at] = product(dest, core, n)
        to_peer(b, R_P).start()

    def chip_sum(b):
        at = rows_of(b, OWN)
        total = p_own[at, :] + p_rcv[at, :].astype(jnp.float32)
        p_own[at, :] = total
        c_buf[at, :] = total.astype(jnp.bfloat16)

    own[0].wait_recv()
    fwd[0].start()

    wait_received(R_P, 3 * OWN)

    @pl.loop(0, 3)
    def _(b):
        chip_sum(b)

    def c_half(b, h):
        return c_buf.at[(2 * b + h) * HALF:(2 * b + h + 1) * HALF]

    far = [copy(c_half(0, h), rs_far.at[h], S_MAIN, R_FAR + h, chain) for h in range(2)]
    one = [
        copy(c_buf.at[3 * OWN + i:3 * OWN + j], rs_one.at[i:j], S_P, R_ONE + n, beside)
        for n, (i, j) in enumerate(CHUNKS)
    ]
    whole = [copy(rs_snd.at[h], rs_sum.at[h * HALF:(h + 1) * HALF], S_P, R_SUM + h, chain) for h in range(2)]

    for item in far:
        item.start()

    turned.wait_recv()
    shares = [copy(quarter, quarter, S_SHARE, R_SHARE, cross) for cross in crosses]

    @pl.when(core == 1)
    def _():
        pl.semaphore_wait(told, 1)

    for share in shares:
        share.start()
    own[1].wait_recv()
    fwd[1].start()
    swap(zs).start()

    wait_received(R_SHARE, 3 * HALF)
    turned.wait_send()
    ogt[rows_of(zo, 2 * OWN), :] = ogt_pair[...]
    for n in range(4):
        at = slice(n * 256, (n + 1) * 256)
        p_snd[3 * OWN:, at] = product(zo, other, n).astype(jnp.bfloat16)
    for n in range(4):
        at = slice(n * 256, (n + 1) * 256)
        p_own[3 * OWN:, at] = product(zo, core, n)
    last = to_peer(3, R_P3)
    last.start()
    for k in range(ROWS // 128):
        at = slice(k * 128, (k + 1) * 128)
        og[:, at] = jnp.transpose(ogt[at, :])
    last.wait_recv()
    chip_sum(3)

    one[0].start()
    wait_received(R_ASIDE, OWN)
    swap(zo).start()
    wait_received(R_FWD, OWN)
    swap(zf).start()
    wait_received(R_SWAP, 4 * OWN)

    def g_half(j, h):
        return g.at[rows_of(j * 2 + h, SUB)]

    far_p = copy(g_half(yf, hp), y_far.at[0], S_Y, R_FP, way_p)
    far_m = copy(g_half(yf, zl), y_far.at[1], S_Y, R_FM, way_m)
    own_p = copy(g_half(ym, hp), y_own.at[0], S_Y, R_PP, way_m)
    own_m = copy(g_half(yp, zl), y_own.at[1], S_Y, R_MM, way_p)
    sum_p = copy(y_snd.at[0], y_sum.at[0], S_Y, R_PP, way_p)
    sum_m = copy(y_snd.at[1], y_sum.at[1], S_Y, R_MM, way_m)

    def block(t, n):
        return jnp.dot(
            og[rows_of(t, 2 * SUB), :], q[:, n * 256:(n + 1) * 256],
            preferred_element_type=jnp.float32,
        )

    @pl.loop(0, 3)
    def _(k):
        t = jnp.where(k == 0, yf, jnp.where(k == 1, ym, yp))
        for n in range(4):
            g[rows_of(t, 2 * SUB), n * 256:(n + 1) * 256] = block(t, n).astype(jnp.bfloat16)

        @pl.when(k == 0)
        def _():
            far_p.start()
            far_m.start()

        @pl.when(k == 1)
        def _():
            own_p.start()

    for n in range(4):
        gown[:, n * 256:(n + 1) * 256] = block(y, n)

    def middle(h):
        far[h].wait_recv()
        rs_snd[h] = (
            p_own[OWN + h * HALF:OWN + (h + 1) * HALF, :] + rs_far[h].astype(jnp.float32)
        ).astype(jnp.bfloat16)
        whole[h].start()

    middle(0)
    far_p.wait_recv()
    y_snd[0] = (
        g[rows_of(yp * 2 + hp, SUB), :].astype(jnp.float32) + y_far[0].astype(jnp.float32)
    ).astype(jnp.bfloat16)
    sum_p.start()
    own_m.start()

    far_m.wait_recv()
    y_snd[1] = (
        g[rows_of(ym * 2 + zl, SUB), :].astype(jnp.float32) + y_far[1].astype(jnp.float32)
    ).astype(jnp.bfloat16)
    sum_m.start()
    middle(1)
    one[1].start()
    one[2].start()

    wait_received(R_PP, 2 * SUB)
    z_snd[...] = (
        gown[rows_of(hp, SUB), :] + y_own[0].astype(jnp.float32) + y_sum[0].astype(jnp.float32)
    ).astype(jnp.bfloat16)
    across = copy(z_snd, z_rcv, S_Y, R_Z, pair)
    across.start()
    wait_received(R_MM, 2 * SUB)
    mine[...] = (
        gown[rows_of(zl, SUB), :] + y_own[1].astype(jnp.float32) + y_sum[1].astype(jnp.float32)
    )

    def finish(n):
        i, j = CHUNKS[n]
        one[n].wait_recv()
        part = jnp.zeros((j - i, 128), jnp.float32)
        for k in range(COLS // 128):
            at = slice(k * 128, (k + 1) * 128)
            summed = (
                p_own[2 * OWN + i:2 * OWN + j, at]
                + rs_one[i:j, at].astype(jnp.float32) + rs_sum[i:j, at].astype(jnp.float32)
            )
            wg_out[i:j, at] = summed * ins[i:j, at]
            part = part + summed * fac[i:j, at]
        parts[i:j, :] = part

    def row_sums(h):
        at = slice(h * 128, (h + 1) * 128)
        x_snd[:, at] = jnp.broadcast_to(
            jnp.sum(jnp.transpose(parts[at, :]), axis=0, keepdims=True) * GRAD_FACTOR, (8, 128)
        )

    parts[OWN:, :] = jnp.zeros((256 - OWN, 128), jnp.float32)
    whole[0].wait_recv()
    finish(0)
    whole[1].wait_recv()
    finish(1)
    row_sums(0)
    finish(2)
    row_sums(1)
    sends = [copy(x_snd, x_rcv.at[k], S_X, R_X, crosses[k]) for k in range(3)]
    for send in sends:
        send.start()

    across.wait_recv()
    ig_out[...] = (mine[...] + z_rcv[...].astype(jnp.float32)).astype(jnp.bfloat16)

    wait_sent(S_MAIN, ROWS)
    wait_sent(S_P, 6 * OWN)
    wait_sent(S_Y, 7 * SUB)
    wait_sent(S_SHARE, 3 * HALF)

    both = copy(x_rcv, x_rcv, S_X, R_X, peer)
    both.wait_recv()
    total = x_snd[...] + x_rcv[0] + x_rcv[1] + x_rcv[2]
    sg_out[...] = total[0:1, 0:OWN]
    both.wait_send()


def store(ig_ref, wg_ref, sg_ref, ig_hbm, wg_hbm, sg_hbm, sems):
    moves = [
        pltpu.make_async_copy(wg_ref.at[i:i + 56], wg_hbm.at[i:i + 56], sems.at[i // 56])
        for i in range(0, OWN, 56)
    ] + [
        pltpu.make_async_copy(ig_ref, ig_hbm, sems.at[4]),
        pltpu.make_async_copy(sg_ref, sg_hbm, sems.at[5]),
    ]
    for move in moves:
        move.start()
    for move in moves:
        move.wait()


def shards(activations, out_grad, weight, step_size):
    bf16, f32 = jnp.bfloat16, jnp.float32
    hbm = pl.BlockSpec(memory_space=pltpu.HBM)
    vmem = pl.BlockSpec(memory_space=pltpu.VMEM)
    input_grad, weight_grad, step_rows = pl.pallas_call(
        kernel,
        out_shape=(
            pltpu.VMEM((SUB, COLS), bf16),
            pltpu.VMEM((OWN, COLS), f32),
            pltpu.VMEM((1, OWN), f32),
        ),
        in_specs=[hbm] * 4,
        out_specs=(vmem, vmem, vmem),
        scratch_shapes=[
            pltpu.VMEM((TOKENS, COLS), bf16),
            pltpu.VMEM((TOKENS, ROWS), bf16),
            pltpu.VMEM((OWN, COLS), f32),
            pltpu.VMEM((1, ROWS), f32),
            pltpu.VMEM((3 * 128, 128), f32),
            pltpu.VMEM((ROWS, TOKENS), bf16),
            pltpu.VMEM((2 * OWN, TOKENS), bf16),
            pltpu.VMEM((ROWS, COLS), bf16),
            pltpu.VMEM((OWN, COLS), f32),
            pltpu.VMEM((OWN, COLS), f32),
            pltpu.VMEM((4 * OWN, COLS), f32),
            pltpu.VMEM((4 * OWN, COLS), bf16),
            pltpu.VMEM((4 * OWN, COLS), bf16),
            pltpu.VMEM((4 * OWN, COLS), bf16),
            pltpu.VMEM((2, HALF, COLS), bf16),
            pltpu.VMEM((OWN, COLS), bf16),
            pltpu.VMEM((OWN, COLS), bf16),
            pltpu.VMEM((2, HALF, COLS), bf16),
            pltpu.VMEM((256, 128), f32),
            pltpu.VMEM((TOKENS, COLS), bf16),
            pltpu.VMEM((2 * SUB, COLS), f32),
            pltpu.VMEM((2, SUB, COLS), bf16),
            pltpu.VMEM((2, SUB, COLS), bf16),
            pltpu.VMEM((2, SUB, COLS), bf16),
            pltpu.VMEM((2, SUB, COLS), bf16),
            pltpu.VMEM((SUB, COLS), f32),
            pltpu.VMEM((SUB, COLS), bf16),
            pltpu.VMEM((SUB, COLS), bf16),
            pltpu.VMEM((8, 256), f32),
            pltpu.VMEM((3, 8, 256), f32),
            pltpu.SemaphoreType.DMA((N_SEND,)),
            pltpu.SemaphoreType.DMA((N_RECV,)),
            pltpu.SemaphoreType.DMA((5,)),
            pltpu.SemaphoreType.REGULAR,
        ],
        compiler_params=pltpu.CompilerParams(
            collective_id=0, has_side_effects=True, vmem_limit_bytes=60*1024*1024
        ),
        name="backward",
    )(activations, out_grad, weight[0], step_size)
    outs = pl.pallas_call(
        store,
        out_shape=(
            jax.ShapeDtypeStruct((SUB, COLS), bf16),
            jax.ShapeDtypeStruct((OWN, COLS), f32),
            jax.ShapeDtypeStruct((1, OWN), f32),
        ),
        in_specs=[vmem] * 3,
        out_specs=(hbm,) * 3,
        scratch_shapes=[pltpu.SemaphoreType.DMA((6,))],
        compiler_params=pltpu.CompilerParams(vmem_limit_bytes=4 * 1024 * 1024),
        name="store",
    )(input_grad, weight_grad, step_rows)
    return (outs[0], outs[1][None], outs[2])


def solution(mesh):
    split = Mesh(mesh.devices.reshape(4, 2, 4, 2, 4), ("zh", "core", "y", "zl", "x"))
    in_specs = (P(DP, "x"), P(DP, ROW), P(ROW, DP, "x"), P(ROW, None))
    out_specs = (P(DP + ROW, "x"), P(ROW, DP, "x"), P(ROW, DP))
    return jax.shard_map(
        shards, mesh=split, in_specs=in_specs, out_specs=out_specs, check_vma=False
    )
```

```python
import functools

import jax
import jax.numpy as jnp
from jax import lax
from jax.experimental import pallas as pl
from jax.experimental.pallas import tpu as pltpu
from jax.sharding import Mesh
from jax.sharding import PartitionSpec as P

MESH = pl.DeviceIdType.MESH
D = 4096
DP = ("zh", "core")
ROW = ("y", "zl")
OWN = 224
HALF = 112
COLS = 1024
ROWS = 1792
TOKENS = 1024
SUB = 128
CHUNKS = ((0, 112), (112, 192), (192, 224))
GRAD_FACTOR = 1.0 / (7.0 * D) ** 0.5

S_MAIN, S_P, S_Y, S_SHARE, S_TURN, S_X, N_SEND = range(7)
(
    R_OWN, _, R_FWD, R_ASIDE, R_SWAP, R_P, R_P3, R_FAR, _, R_SUM, _, R_ONE, _, _,
    R_FP, R_FM, R_PP, R_MM, R_Z, R_X, R_TURN, R_SHARE, N_RECV,
) = range(23)


def rows_of(index, size):
    return pl.ds(pl.multiple_of(index * size, size), size)


def kernel(
    act_hbm, og_hbm, w_hbm, s_hbm,
    ig_out, wg_out, sg_out,
    act, og, w, s, scol, ogt, ogt_pair, q, fac, ins,
    p_own, p_snd, p_rcv, c_buf,
    rs_far, rs_one, rs_sum, rs_snd, parts,
    g, gown, y_far, y_own, y_sum, y_snd, mine, z_snd, z_rcv,
    x_snd, x_rcv,
    ss, rs, ls, told,
):
    zh = lax.axis_index("zh")
    core = lax.axis_index("core")
    y = lax.axis_index("y")
    zl = lax.axis_index("zl")
    x = lax.axis_index("x")
    zf = (zh + 2) % 4
    zs = (zh + 3 + 2 * zl) % 4
    zo = (zh + 1 + 2 * zl) % 4
    chain, back = {"zh": zs}, {"zh": zo}
    beside = {"zh": zs, "zl": 1 - zl}
    other = 1 - core
    peer = {"core": other}
    yf = (y + 2) % 4
    pair = {"zl": 1 - zl}
    crosses = [{"x": (x + k) % 4} for k in (2, 1, 3)]
    hp = 1 - zl
    yp = (y + 1 + 2 * hp) % 4
    ym = (y + 3 + 2 * hp) % 4
    way_p, way_m = {"y": yp}, {"y": ym}

    loads = [
        pltpu.make_async_copy(s_hbm, s, ls.at[0]),
        pltpu.make_async_copy(w_hbm.at[0:HALF], w.at[0:HALF], ls.at[1]),
        pltpu.make_async_copy(w_hbm.at[HALF:OWN], w.at[HALF:OWN], ls.at[2]),
        pltpu.make_async_copy(og_hbm, og, ls.at[3]),
        pltpu.make_async_copy(act_hbm, act, ls.at[4]),
    ]
    barrier = pltpu.get_barrier_semaphore()
    near = [beside, peer]
    others = [chain, back, pair, way_p, way_m] + crosses
    for partner in near:
        pl.semaphore_signal(barrier, inc=1, device_id=partner, device_id_type=MESH)
    for partner in others:
        pl.semaphore_signal(barrier, inc=1, device_id={**partner, "core": 0}, device_id_type=MESH)

    loads[0].start()
    loads[1].start()

    def copy(src, dst, sender, receiver, device):
        return pltpu.make_async_remote_copy(
            src_ref=src, dst_ref=dst, send_sem=ss.at[sender], recv_sem=rs.at[receiver],
            device_id=device, device_id_type=MESH,
        )

    def wait_received(receiver, rows):
        copy(q.at[0:rows], q.at[0:rows], S_MAIN, receiver, peer).wait_recv()

    def wait_sent(sender, rows):
        copy(q.at[0:rows], q.at[0:rows], sender, R_SWAP, peer).wait_send()

    def shard(j):
        return q.at[rows_of(j * 2 + core, OWN)]

    def half(j, h):
        return q.at[rows_of((j * 2 + core) * 2 + h, HALF)]

    first_row = (zh * 2 + core) * OWN
    tile = jnp.minimum(first_row // 128, (ROWS - 3 * 128) // 128)
    loads[0].wait()
    loads[2].start()
    scol[...] = jnp.transpose(
        jnp.broadcast_to(s[:, pl.ds(pl.multiple_of(tile * 128, 128), 3 * 128)], (128, 3 * 128))
    )
    scale_at = first_row - tile * 128

    def quantize(h):
        rows = slice(h * HALF, (h + 1) * HALF)
        scale = scol[pl.ds(pl.multiple_of(scale_at + h * HALF, 16), HALF), :]
        for k in range(COLS // 128):
            at = slice(k * 128, (k + 1) * 128)
            levels = jnp.floor(jnp.clip(w[rows, at] / scale, -8.0, 7.0) + 0.5)
            q[rows_of((zh * 2 + core) * 2 + h, HALF), at] = (levels * scale).astype(jnp.bfloat16)

    loads[1].wait()
    quantize(0)

    @pl.when(core == 1)
    def _():
        pl.semaphore_wait(barrier, len(near))

    @pl.when(core == 0)
    def _():
        pl.semaphore_wait(barrier, len(near) + 2 * len(others))
        pl.semaphore_signal(told, inc=1, device_id=peer, device_id_type=MESH)

    own = [copy(half(zh, h), half(zh, h), S_MAIN, R_OWN + h, back) for h in range(2)]
    fwd = [copy(half(zs, h), half(zs, h), S_MAIN, R_FWD, back) for h in range(2)]
    aside = [copy(half(zh, h), half(zf, h), S_MAIN, R_ASIDE, beside) for h in range(2)]

    def swap(j):
        return copy(shard(j), shard(j), S_MAIN, R_SWAP, peer)

    aside[0].start()
    loads[3].start()
    loads[4].start()
    loads[2].wait()
    quantize(1)

    @pl.when(core == 1)
    def _():
        pl.semaphore_wait(told, 1)

    own[0].start()

    loads[3].wait()
    aside[1].start()
    swap(zh).start()
    for k in range(ROWS // 128):
        at = slice(k * 128, (k + 1) * 128)
        ogt[at, :] = jnp.transpose(og[:, at])

    quarter = ogt_pair.at[rows_of(x, HALF)]
    turned = copy(ogt.at[rows_of(zo * 4 + x, HALF)], quarter, S_TURN, R_TURN, pair)
    turned.start()
    own[1].start()

    scale = scol[pl.ds(pl.multiple_of(scale_at, 16), OWN), :]
    for k in range(COLS // 128):
        at = slice(k * 128, (k + 1) * 128)
        ratio = w[:, at] / scale
        clipped = jnp.clip(ratio, -8.0, 7.0)
        levels = jnp.floor(clipped + 0.5)
        inside = (ratio >= -8.0) & (ratio <= 7.0)
        ins[:, at] = jnp.where(inside, 1.0, 0.0)
        fac[:, at] = jnp.where(inside, levels - ratio, clipped)

    loads[4].wait()

    def product(at, c, n):
        return jnp.dot(
            ogt[rows_of(at * 2 + c, OWN), :], act[:, n * 256:(n + 1) * 256],
            preferred_element_type=jnp.float32,
        )

    def to_peer(b, receiver):
        return copy(
            p_snd.at[rows_of(b, OWN)], p_rcv.at[rows_of(b, OWN)], S_P, receiver, peer
        )

    @pl.loop(0, 3)
    def _(b):
        dest = jnp.where(b == 0, zf, jnp.where(b == 1, zs, zh))
        for n in range(4):
            at = slice(n * 256, (n + 1) * 256)
            p_snd[rows_of(b, OWN), at] = product(dest, other, n).astype(jnp.bfloat16)
        for n in range(4):
            at = slice(n * 256, (n + 1) * 256)
            p_own[rows_of(b, OWN), at] = product(dest, core, n)
        to_peer(b, R_P).start()

    def chip_sum(b):
        at = rows_of(b, OWN)
        total = p_own[at, :] + p_rcv[at, :].astype(jnp.float32)
        p_own[at, :] = total
        c_buf[at, :] = total.astype(jnp.bfloat16)

    own[0].wait_recv()
    fwd[0].start()

    wait_received(R_P, 3 * OWN)

    @pl.loop(0, 3)
    def _(b):
        chip_sum(b)

    def c_half(b, h):
        return c_buf.at[(2 * b + h) * HALF:(2 * b + h + 1) * HALF]

    far = [copy(c_half(0, h), rs_far.at[h], S_MAIN, R_FAR + h, chain) for h in range(2)]
    one = [
        copy(c_buf.at[3 * OWN + i:3 * OWN + j], rs_one.at[i:j], S_P, R_ONE + n, beside)
        for n, (i, j) in enumerate(CHUNKS)
    ]
    whole = [copy(rs_snd.at[h], rs_sum.at[h * HALF:(h + 1) * HALF], S_P, R_SUM + h, chain) for h in range(2)]

    for item in far:
        item.start()

    turned.wait_recv()
    shares = [copy(quarter, quarter, S_SHARE, R_SHARE, cross) for cross in crosses]
    for share in shares:
        share.start()
    own[1].wait_recv()
    fwd[1].start()
    swap(zs).start()

    wait_received(R_SHARE, 3 * HALF)
    turned.wait_send()
    ogt[rows_of(zo, 2 * OWN), :] = ogt_pair[...]
    for n in range(4):
        at = slice(n * 256, (n + 1) * 256)
        p_snd[3 * OWN:, at] = product(zo, other, n).astype(jnp.bfloat16)
    for n in range(4):
        at = slice(n * 256, (n + 1) * 256)
        p_own[3 * OWN:, at] = product(zo, core, n)
    last = to_peer(3, R_P3)
    last.start()
    for k in range(ROWS // 128):
        at = slice(k * 128, (k + 1) * 128)
        og[:, at] = jnp.transpose(ogt[at, :])
    last.wait_recv()
    chip_sum(3)

    one[0].start()
    wait_received(R_ASIDE, OWN)
    swap(zo).start()
    wait_received(R_FWD, OWN)
    swap(zf).start()
    wait_received(R_SWAP, 4 * OWN)

    def g_half(j, h):
        return g.at[rows_of(j * 2 + h, SUB)]

    far_p = copy(g_half(yf, hp), y_far.at[0], S_Y, R_FP, way_p)
    far_m = copy(g_half(yf, zl), y_far.at[1], S_Y, R_FM, way_m)
    own_p = copy(g_half(ym, hp), y_own.at[0], S_Y, R_PP, way_m)
    own_m = copy(g_half(yp, zl), y_own.at[1], S_Y, R_MM, way_p)
    sum_p = copy(y_snd.at[0], y_sum.at[0], S_Y, R_PP, way_p)
    sum_m = copy(y_snd.at[1], y_sum.at[1], S_Y, R_MM, way_m)

    def block(t, n):
        return jnp.dot(
            og[rows_of(t, 2 * SUB), :], q[:, n * 256:(n + 1) * 256],
            preferred_element_type=jnp.float32,
        )

    @pl.loop(0, 3)
    def _(k):
        t = jnp.where(k == 0, yf, jnp.where(k == 1, ym, yp))
        for n in range(4):
            g[rows_of(t, 2 * SUB), n * 256:(n + 1) * 256] = block(t, n).astype(jnp.bfloat16)

        @pl.when(k == 0)
        def _():
            far_p.start()
            far_m.start()

        @pl.when(k == 1)
        def _():
            own_p.start()

    for n in range(4):
        gown[:, n * 256:(n + 1) * 256] = block(y, n)

    def middle(h):
        far[h].wait_recv()
        rs_snd[h] = (
            p_own[OWN + h * HALF:OWN + (h + 1) * HALF, :] + rs_far[h].astype(jnp.float32)
        ).astype(jnp.bfloat16)
        whole[h].start()

    middle(0)
    far_p.wait_recv()
    y_snd[0] = (
        g[rows_of(yp * 2 + hp, SUB), :].astype(jnp.float32) + y_far[0].astype(jnp.float32)
    ).astype(jnp.bfloat16)
    sum_p.start()
    own_m.start()

    far_m.wait_recv()
    y_snd[1] = (
        g[rows_of(ym * 2 + zl, SUB), :].astype(jnp.float32) + y_far[1].astype(jnp.float32)
    ).astype(jnp.bfloat16)
    sum_m.start()
    middle(1)
    one[1].start()
    one[2].start()

    wait_received(R_PP, 2 * SUB)
    z_snd[...] = (
        gown[rows_of(hp, SUB), :] + y_own[0].astype(jnp.float32) + y_sum[0].astype(jnp.float32)
    ).astype(jnp.bfloat16)
    across = copy(z_snd, z_rcv, S_Y, R_Z, pair)
    across.start()
    wait_received(R_MM, 2 * SUB)
    mine[...] = (
        gown[rows_of(zl, SUB), :] + y_own[1].astype(jnp.float32) + y_sum[1].astype(jnp.float32)
    )

    def finish(n):
        i, j = CHUNKS[n]
        one[n].wait_recv()
        part = jnp.zeros((j - i, 128), jnp.float32)
        for k in range(COLS // 128):
            at = slice(k * 128, (k + 1) * 128)
            summed = (
                p_own[2 * OWN + i:2 * OWN + j, at]
                + rs_one[i:j, at].astype(jnp.float32) + rs_sum[i:j, at].astype(jnp.float32)
            )
            wg_out[i:j, at] = summed * ins[i:j, at]
            part = part + summed * fac[i:j, at]
        parts[i:j, :] = part

    def row_sums(h):
        at = slice(h * 128, (h + 1) * 128)
        x_snd[:, at] = jnp.sum(jnp.transpose(parts[at, :]), axis=0, keepdims=True) * GRAD_FACTOR

    parts[OWN:, :] = jnp.zeros((256 - OWN, 128), jnp.float32)
    whole[0].wait_recv()
    finish(0)
    whole[1].wait_recv()
    finish(1)
    row_sums(0)
    finish(2)
    row_sums(1)
    sends = [copy(x_snd, x_rcv.at[k], S_X, R_X, crosses[k]) for k in range(3)]
    for send in sends:
        send.start()

    across.wait_recv()
    ig_out[...] = (mine[...] + z_rcv[...].astype(jnp.float32)).astype(jnp.bfloat16)

    wait_sent(S_MAIN, ROWS)
    wait_sent(S_P, 6 * OWN)
    wait_sent(S_Y, 7 * SUB)
    wait_sent(S_SHARE, 3 * HALF)

    both = copy(x_rcv, x_rcv, S_X, R_X, peer)
    both.wait_recv()
    total = x_snd[...] + x_rcv[0] + x_rcv[1] + x_rcv[2]
    sg_out[...] = total[:, 0:OWN]
    both.wait_send()


def store(ig_ref, wg_ref, sg_ref, ig_hbm, wg_hbm, sg_hbm, sems):
    moves = [
        pltpu.make_async_copy(wg_ref.at[i:i + 56], wg_hbm.at[i:i + 56], sems.at[i // 56])
        for i in range(0, OWN, 56)
    ] + [
        pltpu.make_async_copy(ig_ref, ig_hbm, sems.at[4]),
        pltpu.make_async_copy(sg_ref, sg_hbm, sems.at[5]),
    ]
    for move in moves:
        move.start()
    for move in moves:
        move.wait()


def shards(activations, out_grad, weight, step_size):
    bf16, f32 = jnp.bfloat16, jnp.float32
    hbm = pl.BlockSpec(memory_space=pltpu.HBM)
    vmem = pl.BlockSpec(memory_space=pltpu.VMEM)
    input_grad, weight_grad, step_rows = pl.pallas_call(
        kernel,
        out_shape=(
            pltpu.VMEM((SUB, COLS), bf16),
            pltpu.VMEM((OWN, COLS), f32),
            pltpu.VMEM((1, OWN), f32),
        ),
        in_specs=[hbm] * 4,
        out_specs=(vmem, vmem, vmem),
        scratch_shapes=[
            pltpu.VMEM((TOKENS, COLS), bf16),
            pltpu.VMEM((TOKENS, ROWS), bf16),
            pltpu.VMEM((OWN, COLS), f32),
            pltpu.VMEM((1, ROWS), f32),
            pltpu.VMEM((3 * 128, 128), f32),
            pltpu.VMEM((ROWS, TOKENS), bf16),
            pltpu.VMEM((2 * OWN, TOKENS), bf16),
            pltpu.VMEM((ROWS, COLS), bf16),
            pltpu.VMEM((OWN, COLS), f32),
            pltpu.VMEM((OWN, COLS), f32),
            pltpu.VMEM((4 * OWN, COLS), f32),
            pltpu.VMEM((4 * OWN, COLS), bf16),
            pltpu.VMEM((4 * OWN, COLS), bf16),
            pltpu.VMEM((4 * OWN, COLS), bf16),
            pltpu.VMEM((2, HALF, COLS), bf16),
            pltpu.VMEM((OWN, COLS), bf16),
            pltpu.VMEM((OWN, COLS), bf16),
            pltpu.VMEM((2, HALF, COLS), bf16),
            pltpu.VMEM((256, 128), f32),
            pltpu.VMEM((TOKENS, COLS), bf16),
            pltpu.VMEM((2 * SUB, COLS), f32),
            pltpu.VMEM((2, SUB, COLS), bf16),
            pltpu.VMEM((2, SUB, COLS), bf16),
            pltpu.VMEM((2, SUB, COLS), bf16),
            pltpu.VMEM((2, SUB, COLS), bf16),
            pltpu.VMEM((SUB, COLS), f32),
            pltpu.VMEM((SUB, COLS), bf16),
            pltpu.VMEM((SUB, COLS), bf16),
            pltpu.VMEM((1, 256), f32),
            pltpu.VMEM((3, 1, 256), f32),
            pltpu.SemaphoreType.DMA((N_SEND,)),
            pltpu.SemaphoreType.DMA((N_RECV,)),
            pltpu.SemaphoreType.DMA((5,)),
            pltpu.SemaphoreType.REGULAR,
        ],
        compiler_params=pltpu.CompilerParams(
            collective_id=0, has_side_effects=True, vmem_limit_bytes=60*1024*1024
        ),
        name="backward",
    )(activations, out_grad, weight[0], step_size)
    outs = pl.pallas_call(
        store,
        out_shape=(
            jax.ShapeDtypeStruct((SUB, COLS), bf16),
            jax.ShapeDtypeStruct((OWN, COLS), f32),
            jax.ShapeDtypeStruct((1, OWN), f32),
        ),
        in_specs=[vmem] * 3,
        out_specs=(hbm,) * 3,
        scratch_shapes=[pltpu.SemaphoreType.DMA((6,))],
        compiler_params=pltpu.CompilerParams(vmem_limit_bytes=4 * 1024 * 1024),
        name="store",
    )(input_grad, weight_grad, step_rows)
    return (outs[0], outs[1][None], outs[2])


def solution(mesh):
    split = Mesh(mesh.devices.reshape(4, 2, 4, 2, 4), ("zh", "core", "y", "zl", "x"))
    in_specs = (P(DP, "x"), P(DP, ROW), P(ROW, DP, "x"), P(ROW, None))
    out_specs = (P(DP + ROW, "x"), P(ROW, DP, "x"), P(ROW, DP))
    return jax.shard_map(
        shards, mesh=split, in_specs=in_specs, out_specs=out_specs, check_vma=False
    )
```

```python
import functools

import jax
import jax.numpy as jnp
from jax import lax
from jax.experimental import pallas as pl
from jax.experimental.pallas import tpu as pltpu
from jax.sharding import Mesh
from jax.sharding import PartitionSpec as P

MESH = pl.DeviceIdType.MESH
D = 4096
DP = ("zh", "core")
ROW = ("y", "zl")
OWN = 224
HALF = 112
COLS = 1024
ROWS = 1792
TOKENS = 1024
SUB = 128
CHUNKS = ((0, 112), (112, 192), (192, 224))
GRAD_FACTOR = 1.0 / (7.0 * D) ** 0.5

S_MAIN, S_P, S_Y, S_SHARE, S_TURN, S_X, N_SEND = range(7)
(
    R_OWN, _, R_FWD, R_ASIDE, R_SWAP, R_P, R_P3, R_FAR, _, R_SUM, _, R_ONE, _, _,
    R_FP, R_FM, R_PP, R_MM, R_Z, R_X, R_TURN, R_SHARE, N_RECV,
) = range(23)


def rows_of(index, size):
    return pl.ds(pl.multiple_of(index * size, size), size)


def kernel(
    act_hbm, og_hbm, w_hbm, s_hbm,
    ig_out, wg_out, sg_out,
    act, og, w, s, scol, ogt, ogt_pair, q, fac, ins,
    p_own, p_snd, p_rcv, c_buf,
    rs_far, rs_one, rs_sum, rs_snd, parts,
    g, gown, y_far, y_own, y_sum, y_snd, mine, z_snd, z_rcv,
    x_snd, x_rcv,
    ss, rs, ls, told,
):
    zh = lax.axis_index("zh")
    core = lax.axis_index("core")
    y = lax.axis_index("y")
    zl = lax.axis_index("zl")
    x = lax.axis_index("x")
    zf = (zh + 2) % 4
    zs = (zh + 3 + 2 * zl) % 4
    zo = (zh + 1 + 2 * zl) % 4
    chain, back = {"zh": zs}, {"zh": zo}
    beside = {"zh": zs, "zl": 1 - zl}
    other = 1 - core
    peer = {"core": other}
    yf = (y + 2) % 4
    pair = {"zl": 1 - zl}
    crosses = [{"x": (x + k) % 4} for k in (2, 1, 3)]
    hp = 1 - zl
    yp = (y + 1 + 2 * hp) % 4
    ym = (y + 3 + 2 * hp) % 4
    way_p, way_m = {"y": yp}, {"y": ym}

    loads = [
        pltpu.make_async_copy(s_hbm, s, ls.at[0]),
        pltpu.make_async_copy(w_hbm.at[0:HALF], w.at[0:HALF], ls.at[1]),
        pltpu.make_async_copy(w_hbm.at[HALF:OWN], w.at[HALF:OWN], ls.at[2]),
        pltpu.make_async_copy(og_hbm, og, ls.at[0]),
        pltpu.make_async_copy(act_hbm, act, ls.at[1]),
    ]
    barrier = pltpu.get_barrier_semaphore()
    near = [beside, peer]
    others = [chain, back, pair, way_p, way_m] + crosses
    for partner in near:
        pl.semaphore_signal(barrier, inc=1, device_id=partner, device_id_type=MESH)
    for partner in others:
        pl.semaphore_signal(barrier, inc=1, device_id={**partner, "core": 0}, device_id_type=MESH)

    loads[0].start()
    loads[1].start()

    def copy(src, dst, sender, receiver, device):
        return pltpu.make_async_remote_copy(
            src_ref=src, dst_ref=dst, send_sem=ss.at[sender], recv_sem=rs.at[receiver],
            device_id=device, device_id_type=MESH,
        )

    def wait_received(receiver, rows):
        copy(q.at[0:rows], q.at[0:rows], S_MAIN, receiver, peer).wait_recv()

    def wait_sent(sender, rows):
        copy(q.at[0:rows], q.at[0:rows], sender, R_SWAP, peer).wait_send()

    def shard(j):
        return q.at[rows_of(j * 2 + core, OWN)]

    def half(j, h):
        return q.at[rows_of((j * 2 + core) * 2 + h, HALF)]

    first_row = (zh * 2 + core) * OWN
    tile = jnp.minimum(first_row // 128, (ROWS - 3 * 128) // 128)
    loads[0].wait()
    loads[2].start()
    scol[...] = jnp.transpose(
        jnp.broadcast_to(s[:, pl.ds(pl.multiple_of(tile * 128, 128), 3 * 128)], (128, 3 * 128))
    )
    scale_at = first_row - tile * 128

    def quantize(h):
        rows = slice(h * HALF, (h + 1) * HALF)
        scale = scol[pl.ds(pl.multiple_of(scale_at + h * HALF, 16), HALF), :]
        for k in range(COLS // 128):
            at = slice(k * 128, (k + 1) * 128)
            levels = jnp.floor(jnp.clip(w[rows, at] / scale, -8.0, 7.0) + 0.5)
            q[rows_of((zh * 2 + core) * 2 + h, HALF), at] = (levels * scale).astype(jnp.bfloat16)

    loads[1].wait()
    quantize(0)

    @pl.when(core == 1)
    def _():
        pl.semaphore_wait(barrier, len(near))

    @pl.when(core == 0)
    def _():
        pl.semaphore_wait(barrier, len(near) + 2 * len(others))
        pl.semaphore_signal(told, inc=1, device_id=peer, device_id_type=MESH)

    own = [copy(half(zh, h), half(zh, h), S_MAIN, R_OWN + h, back) for h in range(2)]
    fwd = [copy(half(zs, h), half(zs, h), S_MAIN, R_FWD, back) for h in range(2)]
    aside = [copy(half(zh, h), half(zf, h), S_MAIN, R_ASIDE, beside) for h in range(2)]

    def swap(j):
        return copy(shard(j), shard(j), S_MAIN, R_SWAP, peer)

    aside[0].start()
    loads[3].start()
    loads[4].start()
    loads[2].wait()
    quantize(1)

    @pl.when(core == 1)
    def _():
        pl.semaphore_wait(told, 1)

    own[0].start()

    loads[3].wait()
    aside[1].start()
    swap(zh).start()
    for k in range(ROWS // 128):
        at = slice(k * 128, (k + 1) * 128)
        ogt[at, :] = jnp.transpose(og[:, at])

    quarter = ogt_pair.at[rows_of(x, HALF)]
    turned = copy(ogt.at[rows_of(zo * 4 + x, HALF)], quarter, S_TURN, R_TURN, pair)
    turned.start()
    own[1].start()

    scale = scol[pl.ds(pl.multiple_of(scale_at, 16), OWN), :]
    for k in range(COLS // 128):
        at = slice(k * 128, (k + 1) * 128)
        ratio = w[:, at] / scale
        clipped = jnp.clip(ratio, -8.0, 7.0)
        levels = jnp.floor(clipped + 0.5)
        inside = (ratio >= -8.0) & (ratio <= 7.0)
        ins[:, at] = jnp.where(inside, 1.0, 0.0)
        fac[:, at] = jnp.where(inside, levels - ratio, clipped)

    loads[4].wait()

    def product(at, c, n):
        return jnp.dot(
            ogt[rows_of(at * 2 + c, OWN), :], act[:, n * 256:(n + 1) * 256],
            preferred_element_type=jnp.float32,
        )

    def to_peer(b, receiver):
        return copy(
            p_snd.at[rows_of(b, OWN)], p_rcv.at[rows_of(b, OWN)], S_P, receiver, peer
        )

    @pl.loop(0, 3)
    def _(b):
        dest = jnp.where(b == 0, zf, jnp.where(b == 1, zs, zh))
        for n in range(4):
            at = slice(n * 256, (n + 1) * 256)
            p_snd[rows_of(b, OWN), at] = product(dest, other, n).astype(jnp.bfloat16)
        for n in range(4):
            at = slice(n * 256, (n + 1) * 256)
            p_own[rows_of(b, OWN), at] = product(dest, core, n)
        to_peer(b, R_P).start()

    def chip_sum(b):
        at = rows_of(b, OWN)
        total = p_own[at, :] + p_rcv[at, :].astype(jnp.float32)
        p_own[at, :] = total
        c_buf[at, :] = total.astype(jnp.bfloat16)

    own[0].wait_recv()
    fwd[0].start()

    wait_received(R_P, 3 * OWN)

    @pl.loop(0, 3)
    def _(b):
        chip_sum(b)

    def c_half(b, h):
        return c_buf.at[(2 * b + h) * HALF:(2 * b + h + 1) * HALF]

    far = [copy(c_half(0, h), rs_far.at[h], S_MAIN, R_FAR + h, chain) for h in range(2)]
    one = [
        copy(c_buf.at[3 * OWN + i:3 * OWN + j], rs_one.at[i:j], S_P, R_ONE + n, beside)
        for n, (i, j) in enumerate(CHUNKS)
    ]
    whole = [copy(rs_snd.at[h], rs_sum.at[h * HALF:(h + 1) * HALF], S_P, R_SUM + h, chain) for h in range(2)]

    for item in far:
        item.start()

    turned.wait_recv()
    shares = [copy(quarter, quarter, S_SHARE, R_SHARE, cross) for cross in crosses]
    for share in shares:
        share.start()
    own[1].wait_recv()
    fwd[1].start()
    swap(zs).start()

    wait_received(R_SHARE, 3 * HALF)
    turned.wait_send()
    ogt[rows_of(zo, 2 * OWN), :] = ogt_pair[...]
    for n in range(4):
        at = slice(n * 256, (n + 1) * 256)
        p_snd[3 * OWN:, at] = product(zo, other, n).astype(jnp.bfloat16)
    for n in range(4):
        at = slice(n * 256, (n + 1) * 256)
        p_own[3 * OWN:, at] = product(zo, core, n)
    last = to_peer(3, R_P3)
    last.start()
    for k in range(ROWS // 128):
        at = slice(k * 128, (k + 1) * 128)
        og[:, at] = jnp.transpose(ogt[at, :])
    last.wait_recv()
    chip_sum(3)

    one[0].start()
    wait_received(R_ASIDE, OWN)
    swap(zo).start()
    wait_received(R_FWD, OWN)
    swap(zf).start()
    wait_received(R_SWAP, 4 * OWN)

    def g_half(j, h):
        return g.at[rows_of(j * 2 + h, SUB)]

    far_p = copy(g_half(yf, hp), y_far.at[0], S_Y, R_FP, way_p)
    far_m = copy(g_half(yf, zl), y_far.at[1], S_Y, R_FM, way_m)
    own_p = copy(g_half(ym, hp), y_own.at[0], S_Y, R_PP, way_m)
    own_m = copy(g_half(yp, zl), y_own.at[1], S_Y, R_MM, way_p)
    sum_p = copy(y_snd.at[0], y_sum.at[0], S_Y, R_PP, way_p)
    sum_m = copy(y_snd.at[1], y_sum.at[1], S_Y, R_MM, way_m)

    def block(t, n):
        return jnp.dot(
            og[rows_of(t, 2 * SUB), :], q[:, n * 256:(n + 1) * 256],
            preferred_element_type=jnp.float32,
        )

    @pl.loop(0, 3)
    def _(k):
        t = jnp.where(k == 0, yf, jnp.where(k == 1, ym, yp))
        for n in range(4):
            g[rows_of(t, 2 * SUB), n * 256:(n + 1) * 256] = block(t, n).astype(jnp.bfloat16)

        @pl.when(k == 0)
        def _():
            far_p.start()
            far_m.start()

        @pl.when(k == 1)
        def _():
            own_p.start()

    for n in range(4):
        gown[:, n * 256:(n + 1) * 256] = block(y, n)

    def middle(h):
        far[h].wait_recv()
        rs_snd[h] = (
            p_own[OWN + h * HALF:OWN + (h + 1) * HALF, :] + rs_far[h].astype(jnp.float32)
        ).astype(jnp.bfloat16)
        whole[h].start()

    middle(0)
    far_p.wait_recv()
    y_snd[0] = (
        g[rows_of(yp * 2 + hp, SUB), :].astype(jnp.float32) + y_far[0].astype(jnp.float32)
    ).astype(jnp.bfloat16)
    sum_p.start()
    own_m.start()

    far_m.wait_recv()
    y_snd[1] = (
        g[rows_of(ym * 2 + zl, SUB), :].astype(jnp.float32) + y_far[1].astype(jnp.float32)
    ).astype(jnp.bfloat16)
    sum_m.start()
    middle(1)
    one[1].start()
    one[2].start()

    wait_received(R_PP, 2 * SUB)
    z_snd[...] = (
        gown[rows_of(hp, SUB), :] + y_own[0].astype(jnp.float32) + y_sum[0].astype(jnp.float32)
    ).astype(jnp.bfloat16)
    across = copy(z_snd, z_rcv, S_Y, R_Z, pair)
    across.start()
    wait_received(R_MM, 2 * SUB)
    mine[...] = (
        gown[rows_of(zl, SUB), :] + y_own[1].astype(jnp.float32) + y_sum[1].astype(jnp.float32)
    )

    def finish(n):
        i, j = CHUNKS[n]
        one[n].wait_recv()
        part = jnp.zeros((j - i, 128), jnp.float32)
        for k in range(COLS // 128):
            at = slice(k * 128, (k + 1) * 128)
            summed = (
                p_own[2 * OWN + i:2 * OWN + j, at]
                + rs_one[i:j, at].astype(jnp.float32) + rs_sum[i:j, at].astype(jnp.float32)
            )
            wg_out[i:j, at] = summed * ins[i:j, at]
            part = part + summed * fac[i:j, at]
        parts[i:j, :] = part

    def row_sums(h):
        at = slice(h * 128, (h + 1) * 128)
        x_snd[:, at] = jnp.sum(jnp.transpose(parts[at, :]), axis=0, keepdims=True) * GRAD_FACTOR

    parts[OWN:, :] = jnp.zeros((256 - OWN, 128), jnp.float32)
    whole[0].wait_recv()
    finish(0)
    whole[1].wait_recv()
    finish(1)
    row_sums(0)
    finish(2)
    row_sums(1)
    sends = [copy(x_snd, x_rcv.at[k], S_X, R_X, crosses[k]) for k in range(3)]
    for send in sends:
        send.start()

    across.wait_recv()
    ig_out[...] = (mine[...] + z_rcv[...].astype(jnp.float32)).astype(jnp.bfloat16)

    wait_sent(S_MAIN, ROWS)
    wait_sent(S_P, 6 * OWN)
    wait_sent(S_Y, 7 * SUB)
    wait_sent(S_SHARE, 3 * HALF)

    both = copy(x_rcv, x_rcv, S_X, R_X, peer)
    both.wait_recv()
    total = x_snd[...] + x_rcv[0] + x_rcv[1] + x_rcv[2]
    sg_out[...] = total[:, 0:OWN]
    both.wait_send()


def store(ig_ref, wg_ref, sg_ref, ig_hbm, wg_hbm, sg_hbm, sems):
    moves = [
        pltpu.make_async_copy(wg_ref, wg_hbm, sems.at[0]),
        pltpu.make_async_copy(ig_ref, ig_hbm, sems.at[1]),
        pltpu.make_async_copy(sg_ref, sg_hbm, sems.at[2]),
    ]
    for move in moves:
        move.start()
    for move in moves:
        move.wait()


def shards(activations, out_grad, weight, step_size):
    bf16, f32 = jnp.bfloat16, jnp.float32
    hbm = pl.BlockSpec(memory_space=pltpu.HBM)
    vmem = pl.BlockSpec(memory_space=pltpu.VMEM)
    input_grad, weight_grad, step_rows = pl.pallas_call(
        kernel,
        out_shape=(
            pltpu.VMEM((SUB, COLS), bf16),
            pltpu.VMEM((OWN, COLS), f32),
            pltpu.VMEM((1, OWN), f32),
        ),
        in_specs=[hbm] * 4,
        out_specs=(vmem, vmem, vmem),
        scratch_shapes=[
            pltpu.VMEM((TOKENS, COLS), bf16),
            pltpu.VMEM((TOKENS, ROWS), bf16),
            pltpu.VMEM((OWN, COLS), f32),
            pltpu.VMEM((1, ROWS), f32),
            pltpu.VMEM((3 * 128, 128), f32),
            pltpu.VMEM((ROWS, TOKENS), bf16),
            pltpu.VMEM((2 * OWN, TOKENS), bf16),
            pltpu.VMEM((ROWS, COLS), bf16),
            pltpu.VMEM((OWN, COLS), f32),
            pltpu.VMEM((OWN, COLS), f32),
            pltpu.VMEM((4 * OWN, COLS), f32),
            pltpu.VMEM((4 * OWN, COLS), bf16),
            pltpu.VMEM((4 * OWN, COLS), bf16),
            pltpu.VMEM((4 * OWN, COLS), bf16),
            pltpu.VMEM((2, HALF, COLS), bf16),
            pltpu.VMEM((OWN, COLS), bf16),
            pltpu.VMEM((OWN, COLS), bf16),
            pltpu.VMEM((2, HALF, COLS), bf16),
            pltpu.VMEM((256, 128), f32),
            pltpu.VMEM((TOKENS, COLS), bf16),
            pltpu.VMEM((2 * SUB, COLS), f32),
            pltpu.VMEM((2, SUB, COLS), bf16),
            pltpu.VMEM((2, SUB, COLS), bf16),
            pltpu.VMEM((2, SUB, COLS), bf16),
            pltpu.VMEM((2, SUB, COLS), bf16),
            pltpu.VMEM((SUB, COLS), f32),
            pltpu.VMEM((SUB, COLS), bf16),
            pltpu.VMEM((SUB, COLS), bf16),
            pltpu.VMEM((1, 256), f32),
            pltpu.VMEM((3, 1, 256), f32),
            pltpu.SemaphoreType.DMA((N_SEND,)),
            pltpu.SemaphoreType.DMA((N_RECV,)),
            pltpu.SemaphoreType.DMA((3,)),
            pltpu.SemaphoreType.REGULAR,
        ],
        compiler_params=pltpu.CompilerParams(
            collective_id=0, has_side_effects=True, vmem_limit_bytes=60*1024*1024
        ),
        name="backward",
    )(activations, out_grad, weight[0], step_size)
    outs = pl.pallas_call(
        store,
        out_shape=(
            jax.ShapeDtypeStruct((SUB, COLS), bf16),
            jax.ShapeDtypeStruct((OWN, COLS), f32),
            jax.ShapeDtypeStruct((1, OWN), f32),
        ),
        in_specs=[vmem] * 3,
        out_specs=(hbm,) * 3,
        scratch_shapes=[pltpu.SemaphoreType.DMA((3,))],
        compiler_params=pltpu.CompilerParams(vmem_limit_bytes=4 * 1024 * 1024),
        name="store",
    )(input_grad, weight_grad, step_rows)
    return (outs[0], outs[1][None], outs[2])


def solution(mesh):
    split = Mesh(mesh.devices.reshape(4, 2, 4, 2, 4), ("zh", "core", "y", "zl", "x"))
    in_specs = (P(DP, "x"), P(DP, ROW), P(ROW, DP, "x"), P(ROW, None))
    out_specs = (P(DP + ROW, "x"), P(ROW, DP, "x"), P(ROW, DP))
    return jax.shard_map(
        shards, mesh=split, in_specs=in_specs, out_specs=out_specs, check_vma=False
    )
```
